8 devices in a mesh: data: 8 (over z, y, x, core).
Axes of the slice: x: 2, y: 2, z: 1, core: 2. Of those that a mesh axis runs over, the one named last changes fastest.
Arguments:
- w_one: float32 [32, 512, 1024], P(None, 'data')
- w_two: float32 [32, 1024, 512], P(None, 'data')
- mom_one: float32 [32, 512, 1024], P(None, 'data')
- mom_two: float32 [32, 1024, 512], P(None, 'data')
- x_zero: bfloat16 [12288, 512], P('data')
- y_zero: bfloat16 [12288, 512], P('data')
- x_one: bfloat16 [12288, 512], P('data')
- y_one: bfloat16 [12288, 512], P('data')
Outputs:
- output 1: float32 [32, 512, 1024], P(None, 'data')
- output 2: float32 [32, 1024, 512], P(None, 'data')
- output 3: float32 [32, 512, 1024], P(None, 'data')
- output 4: float32 [32, 1024, 512], P(None, 'data')
- output 5: float32 [12288], P('data')
- output 6: float32 [12288, 512], P('data')
All inputs are finite; a program needn't handle non-finite values.
Results may differ from the reference program's by a relative error of at most 0.00859125.
Values are sent between devices in bfloat16 or wider.
A program may use at most 1 GiB of HBM per device.

```python
import jax
import jax.numpy as jnp
from jax import lax

DATA_DEVS = 8
TOK_DEV = 1536
LAYERS = 32
D_MODEL = 512
D_FF = 1024

BATCH = DATA_DEVS * TOK_DEV
LEARN_RATE = 0.1
MOMENTUM = 0.9


def draw_rows(key_vals, key_shift, centre, spread):
    base_vals = jax.random.normal(key_vals, (DATA_DEVS, TOK_DEV, D_MODEL), jnp.float32)
    col_shift = jax.random.normal(key_shift, (DATA_DEVS, 1, D_MODEL), jnp.float32)
    return (spread * base_vals + centre + 0.5 * col_shift).reshape(BATCH, D_MODEL).astype(jnp.bfloat16)


def setup_inputs(seed: int = 0) -> dict:
    key_list = jax.random.split(jax.random.key(seed), 16)
    w_one = jax.random.normal(key_list[0], (LAYERS, D_MODEL, D_FF), jnp.float32) * D_MODEL ** -0.5
    w_two = jax.random.normal(key_list[1], (LAYERS, D_FF, D_MODEL), jnp.float32) * (D_FF * LAYERS) ** -0.5
    scale_one = 0.3 * (D_MODEL * D_FF * LAYERS) ** -0.5
    row_one = 1.0 + 0.5 * jax.random.normal(key_list[2], (LAYERS, D_MODEL, 1), jnp.float32)
    col_one = jax.random.normal(key_list[3], (LAYERS, 1, D_FF), jnp.float32)
    mom_one = scale_one * (row_one * col_one + 0.5 * jax.random.normal(key_list[4], (LAYERS, D_MODEL, D_FF), jnp.float32))
    scale_two = 0.3 / D_MODEL
    row_two = 1.0 + 0.5 * jax.random.normal(key_list[5], (LAYERS, D_FF, 1), jnp.float32)
    col_two = jax.random.normal(key_list[6], (LAYERS, 1, D_MODEL), jnp.float32)
    mom_two = scale_two * (row_two * col_two + 0.5 * jax.random.normal(key_list[7], (LAYERS, D_FF, D_MODEL), jnp.float32))
    return {
        "w_one": w_one,
        "w_two": w_two,
        "mom_one": mom_one,
        "mom_two": mom_two,
        "x_zero": draw_rows(key_list[8], key_list[9], 0.6, 0.8),
        "y_zero": draw_rows(key_list[10], key_list[11], -0.5, 0.5),
        "x_one": draw_rows(key_list[12], key_list[13], 0.6, 0.8),
        "y_one": draw_rows(key_list[14], key_list[15], -0.5, 0.5),
    }


def run_stack(w_one_b, w_two_b, h_start):
    def layer_step(h_cur, weights):
        w_in, w_out = weights
        act_in = h_cur.astype(jnp.bfloat16)
        pre_act = jnp.dot(act_in, w_in, preferred_element_type=jnp.float32)
        hidden = jax.nn.gelu(pre_act).astype(jnp.bfloat16)
        h_next = h_cur + jnp.dot(hidden, w_out, preferred_element_type=jnp.float32)
        return h_next, (act_in, pre_act, hidden)
    return lax.scan(layer_step, h_start, (w_one_b, w_two_b))


def local_grads(w_one_b, w_two_b, x_rows, y_rows):
    h_end, saved_vals = run_stack(w_one_b, w_two_b, x_rows.astype(jnp.float32))
    d_start = (h_end - y_rows.astype(jnp.float32)) / (BATCH * D_MODEL)

    def back_step(d_state, layer_vals):
        w_in, w_out, act_in, pre_act, hidden = layer_vals
        d_low = d_state.astype(jnp.bfloat16)
        grad_out = jnp.dot(hidden.T, d_low, preferred_element_type=jnp.float32).astype(jnp.bfloat16)
        d_hidden = jnp.dot(d_low, w_out.T, preferred_element_type=jnp.float32)
        d_pre = jax.vjp(jax.nn.gelu, pre_act)[1](d_hidden)[0].astype(jnp.bfloat16)
        grad_in = jnp.dot(act_in.T, d_pre, preferred_element_type=jnp.float32).astype(jnp.bfloat16)
        d_next = d_state + jnp.dot(d_pre, w_in.T, preferred_element_type=jnp.float32)
        return d_next, (grad_in, grad_out)

    act_ins, pre_acts, hiddens = saved_vals
    return lax.scan(back_step, d_start, (w_one_b, w_two_b, act_ins, pre_acts, hiddens), reverse=True)[1]


def reference(w_one, w_two, mom_one, mom_two, x_zero, y_zero, x_one, y_one):
    w_one_b = w_one.astype(jnp.bfloat16)
    w_two_b = w_two.astype(jnp.bfloat16)
    x_dev = x_zero.reshape(DATA_DEVS, TOK_DEV, D_MODEL)
    y_dev = y_zero.reshape(DATA_DEVS, TOK_DEV, D_MODEL)

    def add_device(acc_pair, row_pair):
        grad_in, grad_out = local_grads(w_one_b, w_two_b, row_pair[0], row_pair[1])
        return (acc_pair[0] + grad_in.astype(jnp.float32), acc_pair[1] + grad_out.astype(jnp.float32)), None

    zeros_pair = (jnp.zeros(w_one.shape, jnp.float32), jnp.zeros(w_two.shape, jnp.float32))
    grad_sums = lax.scan(add_device, zeros_pair, (x_dev, y_dev))[0]
    new_mom_one = MOMENTUM * mom_one + grad_sums[0].astype(jnp.bfloat16).astype(jnp.float32)
    new_mom_two = MOMENTUM * mom_two + grad_sums[1].astype(jnp.bfloat16).astype(jnp.float32)
    new_w_one = w_one - LEARN_RATE * new_mom_one
    new_w_two = w_two - LEARN_RATE * new_mom_two
    next_one_b = new_w_one.astype(jnp.bfloat16)
    next_two_b = new_w_two.astype(jnp.bfloat16)

    def device_forward(x_rows):
        return run_stack(next_one_b, next_two_b, x_rows.astype(jnp.float32))[0]

    h_last = lax.map(device_forward, x_one.reshape(DATA_DEVS, TOK_DEV, D_MODEL)).reshape(BATCH, D_MODEL)
    loss_rows = jnp.sum(jnp.square(h_last - y_one.astype(jnp.float32)), axis=1) / (2 * D_MODEL)
    return new_w_one, new_w_two, new_mom_one, new_mom_two, loss_rows, h_last
```

```python
import functools

import jax
import jax.numpy as jnp
from jax import lax
from jax.experimental import pallas as pl
from jax.experimental.pallas import tpu as pltpu
from jax.sharding import PartitionSpec as P

LEARN_RATE = 0.1
MOMENTUM = 0.9
GELU_C = 0.7978845608028654
GELU_K = 0.044715
MESH = pl.DeviceIdType.MESH
F32 = jnp.float32
BF16 = jnp.bfloat16
LAG = 2
SLOTS = 4 * LAG + 1
ANY = pl.BlockSpec(memory_space=pl.ANY)


def place():
    me = lax.axis_index("data")
    core, col, row = me % 2, (me // 2) % 2, me // 4
    return me, core, col, row


def index_of(row, col, core):
    return 4 * row + 2 * col + core


def greet(peers):
    barrier = pltpu.get_barrier_semaphore()
    for peer in peers:
        pl.semaphore_signal(barrier, inc=1, device_id=(peer,), device_id_type=MESH)
    pl.semaphore_wait(barrier, len(peers))


def forward_kernel(train, layers, tile, scale, *refs):
    if train:
        (w1s, w2s, x_in, y_in, d_out, zt_out, at_out, p_out, w1t_out, w2t_out,
         w1, w2, h, xb, send_sem, recv_sem, own_sem, io_sem,
         zt_st, at_st, p_st, w1t_st, w2t_st, st_sem, wt_sem) = refs
    else:
        (w1s, w2s, x_in, h_out, w1, w2, h, xb, send_sem, recv_sem, own_sem, io_sem) = refs
    me, core, col, row = place()
    j_p = index_of(row, col, 1 - core)
    j_x = index_of(row, 1 - col, core)
    j_y = index_of(1 - row, col, core)
    j_d = index_of(1 - row, 1 - col, core)
    p_x = index_of(row, 1 - col, 1 - core)
    p_y = index_of(1 - row, col, 1 - core)
    p_d = index_of(1 - row, 1 - col, 1 - core)
    r1, r2 = w1s.shape[1], w2s.shape[1]
    rows = h.shape[0]
    tiles = rows // tile

    greet((j_p, j_x, j_y))

    def part(which, slot, j):
        if which == 1:
            return w1.at[slot, pl.ds(pl.multiple_of(j * r1, r1), r1)]
        return w2.at[slot, pl.ds(pl.multiple_of(j * r2, r2), r2)]

    sends = (
        (1, me, j_y, j_y), (1, me, j_x, j_x), (1, me, j_p, j_p),
        (2, me, j_x, j_x), (2, me, j_y, j_y), (2, me, j_p, j_p),
        (1, j_y, j_x, j_d), (1, j_y, j_p, p_y), (2, j_x, j_y, j_d), (2, j_x, j_p, p_x),
        (1, j_x, j_p, p_x), (2, j_y, j_p, p_y),
        (1, j_d, j_p, p_d), (2, j_d, j_p, p_d),
    )

    def channel(layer, k, incoming=False):
        slot = layer % SLOTS
        which, out, to, inc = sends[k]
        ref = part(which, slot, inc if incoming else out)
        return pltpu.make_async_remote_copy(
            src_ref=ref, dst_ref=ref, send_sem=send_sem.at[slot, k], recv_sem=recv_sem.at[slot, k],
            device_id=(to,), device_id_type=MESH)

    def start(layer, ks):
        for k in ks:
            channel(layer, k).start()

    def arrive(layer, ks):
        for k in ks:
            channel(layer, k, True).wait_recv()

    def own(layer):
        slot = layer % SLOTS
        return (pltpu.make_async_copy(w1s.at[layer], part(1, slot, me), own_sem.at[slot, 0]),
                pltpu.make_async_copy(w2s.at[layer], part(2, slot, me), own_sem.at[slot, 1]))

    def gather(i):
        def on(layer):
            return jnp.logical_and(layer >= 0, layer < layers)

        @pl.when(on(i))
        def _():
            arrive(i, (2, 5, 7, 9, 10, 11, 12, 13))

        @pl.when(on(i + LAG))
        def _():
            arrive(i + LAG, (6, 8))
            start(i + LAG, (12, 13))

        @pl.when(on(i + 2 * LAG))
        def _():
            arrive(i + 2 * LAG, (0, 1, 3, 4))
            start(i + 2 * LAG, (6, 8, 7, 9, 10, 11))

        @pl.when(on(i + 3 * LAG))
        def _():
            for copy in own(i + 3 * LAG):
                copy.wait()
            start(i + 3 * LAG, (0, 3, 1, 4, 2, 5))

        @pl.when(on(i + 3 * LAG + 1))
        def _():
            for copy in own(i + 3 * LAG + 1):
                copy.start()

    def saved(layer, t, st):
        cols = pl.ds(pl.multiple_of(t * tile, tile), tile)
        return (pltpu.make_async_copy(zt_st.at[st], zt_out.at[layer, :, cols], st_sem.at[st, 0]),
                pltpu.make_async_copy(at_st.at[st], at_out.at[layer, :, cols], st_sem.at[st, 1]),
                pltpu.make_async_copy(p_st.at[st], p_out.at[layer, cols], st_sem.at[st, 2]))

    def turned(layer):
        return (pltpu.make_async_copy(w1t_st, w1t_out.at[layer], wt_sem.at[0]),
                pltpu.make_async_copy(w2t_st, w2t_out.at[layer], wt_sem.at[1]))

    def compute(layer):
        slot = layer % SLOTS

        def one(t, _):
            where = pl.ds(pl.multiple_of(t * tile, tile), tile)
            h_val = h[where, :]
            a_val = h_val.astype(BF16)
            u = jnp.dot(a_val, w1[slot], preferred_element_type=F32)
            sq = u * u
            w = 0.5 * (1.0 + jnp.tanh(u * (GELU_C + (GELU_C * GELU_K) * sq)))
            z = u * w
            z_low = z.astype(BF16)
            if train:
                step = layer * tiles + t
                st = step % 2

                @pl.when(step >= 2)
                def _():
                    for copy in saved((step - 2) // tiles, (step - 2) % tiles, st):
                        copy.wait()

                p_st[st] = w + (z * (1.0 - w)) * (2.0 * GELU_C + (6.0 * GELU_C * GELU_K) * sq)
                zt_st[st] = z_low.T
                at_st[st] = a_val.T
                for copy in saved(layer, t, st):
                    copy.start()
            h[where, :] = h_val + jnp.dot(z_low, w2[slot], preferred_element_type=F32)
            return 0

        lax.fori_loop(0, tiles, one, 0)
        if train:
            @pl.when(layer >= 1)
            def _():
                for copy in turned(layer - 1):
                    copy.wait()

            w1t_st[...] = w1[slot].T
            w2t_st[...] = w2[slot].T
            for copy in turned(layer):
                copy.start()

    x_copy = pltpu.make_async_copy(x_in, xb, io_sem.at[0])
    x_copy.start()
    for copy in own(0):
        copy.start()
    x_copy.wait()

    def widen(t, _):
        where = pl.ds(pl.multiple_of(t * 256, 256), 256)
        h[where, :] = xb[where, :].astype(F32)
        return 0

    lax.fori_loop(0, rows // 256, widen, 0)

    def turn(n, _):
        i = n - 3 * LAG
        gather(i)

        @pl.when(i >= 0)
        def _():
            compute(i)
            for k in range(len(sends)):
                channel(i, k).wait_send()

        return 0

    lax.fori_loop(0, layers + 3 * LAG, turn, 0)

    if train:
        last = layers * tiles
        for step in (last - 2, last - 1):
            for copy in saved(step // tiles, step % tiles, step % 2):
                copy.wait()
        for copy in turned(layers - 1):
            copy.wait()
        y_copy = pltpu.make_async_copy(y_in, xb, io_sem.at[0])
        y_copy.start()
        y_copy.wait()

        def close(t, _):
            where = pl.ds(pl.multiple_of(t * 256, 256), 256)
            h[where, :] = (h[where, :] - xb[where, :].astype(F32)) / scale
            return 0

        lax.fori_loop(0, rows // 256, close, 0)
    out_copy = pltpu.make_async_copy(h, d_out if train else h_out, io_sem.at[1])
    out_copy.start()
    out_copy.wait()


def forward(train, w1s, w2s, x, y=None, scale=None, tile=512, cid=0):
    layers, r1, d_ff = w1s.shape
    r2, d_model = w2s.shape[1:]
    rows = x.shape[0]
    sds = jax.ShapeDtypeStruct
    h_shape = sds((rows, d_model), F32)
    scratch = [
        pltpu.VMEM((SLOTS, d_model, d_ff), BF16), pltpu.VMEM((SLOTS, d_ff, d_model), BF16),
        pltpu.VMEM((rows, d_model), F32), pltpu.VMEM((rows, d_model), BF16),
        pltpu.SemaphoreType.DMA((SLOTS, 14)), pltpu.SemaphoreType.DMA((SLOTS, 14)),
        pltpu.SemaphoreType.DMA((SLOTS, 2)), pltpu.SemaphoreType.DMA((2,)),
    ]
    out = h_shape
    args = (w1s, w2s, x)
    if train:
        out = (h_shape, sds((layers, d_ff, rows), BF16), sds((layers, d_model, rows), BF16),
               sds((layers, rows, d_ff), F32), sds((layers, d_ff, d_model), BF16), sds((layers, d_model, d_ff), BF16))
        args = (w1s, w2s, x, y)
        scratch += [
            pltpu.VMEM((2, d_ff, tile), BF16), pltpu.VMEM((2, d_model, tile), BF16), pltpu.VMEM((2, tile, d_ff), F32),
            pltpu.VMEM((d_ff, d_model), BF16), pltpu.VMEM((d_model, d_ff), BF16),
            pltpu.SemaphoreType.DMA((2, 3)), pltpu.SemaphoreType.DMA((2,)),
        ]
    return pl.pallas_call(
        functools.partial(forward_kernel, train, layers, tile, scale),
        out_shape=out,
        in_specs=[ANY] * len(args),
        out_specs=jax.tree.map(lambda _: ANY, out),
        scratch_shapes=scratch,
        compiler_params=pltpu.CompilerParams(collective_id=cid, has_side_effects=True, vmem_limit_bytes=60 * 2**20),
        name="fwd_train" if train else "fwd_eval",
    )(*args)


WAIT_D, WAIT_1, WAIT_2 = 1, 2, 2


def backward_kernel(layers, tile, *refs):
    (d_in, zt_in, at_in, p_in, w1t_in, w2t_in, g1_out, g2_out,
     d, db, r, zt, at, p, w1t, w2t, ga, gb, da, dbuf, sa, sb, ra, rb, ta, tb, fa, fb, oa, ob,
     in_sem, d_sem, xd_send, xd_recv, x1_send, x1_recv, x2_send, x2_recv, out_sem) = refs
    me, core, col, row = place()
    j_p = index_of(row, col, 1 - core)
    j_x = index_of(row, 1 - col, core)
    j_y = index_of(1 - row, col, core)
    rows = d.shape[0]
    tiles = rows // tile
    n_g, n_r1, n_s, n_r2, n_t = 2, 2 * WAIT_1, WAIT_1 + 1, 2 * WAIT_2, WAIT_2 + 1
    n_d = 2 * WAIT_D
    s1, s2 = ga.shape[4], gb.shape[4]

    greet((j_p, j_x, j_y))

    def loads(n):
        layer, s = layers - 1 - n, n % 2
        return tuple(
            pltpu.make_async_copy(src.at[layer], dst.at[s], in_sem.at[s, k])
            for k, (src, dst) in enumerate(((w2t_in, w2t), (p_in, p), (w1t_in, w1t), (zt_in, zt), (at_in, at))))

    def remote(src, dst, send, recv, to):
        return pltpu.make_async_remote_copy(
            src_ref=src, dst_ref=dst, send_sem=send, recv_sem=recv, device_id=(to,), device_id_type=MESH)

    def hop_d(n):
        g, s = n % n_g, n % n_d
        return (remote(ga.at[g, 1 - core], da.at[s], xd_send.at[s, 0], xd_recv.at[s, 0], j_p),
                remote(gb.at[g, 1 - core], dbuf.at[s], xd_send.at[s, 1], xd_recv.at[s, 1], j_p))

    def hop_1(n):
        g, s = n % n_s, n % n_r1
        return (remote(sa.at[g, 1 - row], ra.at[s], x1_send.at[s, 0], x1_recv.at[s, 0], j_y),
                remote(sb.at[g, 1 - col], rb.at[s], x1_send.at[s, 1], x1_recv.at[s, 1], j_x))

    def hop_2(n):
        g, s = n % n_t, n % n_r2
        return (remote(ta.at[g, 1 - col], fa.at[s], x2_send.at[s, 0], x2_recv.at[s, 0], j_x),
                remote(tb.at[g, 1 - row], fb.at[s], x2_send.at[s, 1], x2_recv.at[s, 1], j_y))

    def results(n):
        layer, s = layers - 1 - n, n % 2
        return (pltpu.make_async_copy(oa.at[s], g1_out.at[layer], out_sem.at[s, 0]),
                pltpu.make_async_copy(ob.at[s], g2_out.at[layer], out_sem.at[s, 1]))

    def on(n):
        return jnp.logical_and(n >= 0, n < layers)

    def add(x, y):
        return (x.astype(F32) + y.astype(F32)).astype(BF16)

    lag_2 = 1 + WAIT_D
    lag_3 = lag_2 + WAIT_1
    lag_4 = lag_3 + WAIT_2

    def exchange(n):
        @pl.when(on(n - lag_4))
        def _():
            m = n - lag_4

            @pl.when(m >= 2)
            def _():
                for copy in results(m - 2):
                    copy.wait()

            for copy in hop_2(m):
                copy.wait()
            oa[m % 2] = add(ta[m % n_t, col], fa[m % n_r2])
            ob[m % 2] = add(tb[m % n_t, row], fb[m % n_r2])
            for copy in results(m):
                copy.start()

        @pl.when(on(n - lag_3))
        def _():
            m = n - lag_3
            for copy in hop_1(m):
                copy.wait()
            ta[m % n_t] = add(sa[m % n_s, row], ra[m % n_r1])
            tb[m % n_t] = add(sb[m % n_s, col], rb[m % n_r1])
            for copy in hop_2(m):
                copy.start()

        @pl.when(on(n - lag_2))
        def _():
            m = n - lag_2
            for copy in hop_d(m):
                copy.wait()
            sa[m % n_s] = add(ga[m % n_g, core], da[m % n_d])
            sb[m % n_s] = add(gb[m % n_g, core], dbuf[m % n_d])
            for copy in hop_1(m):
                copy.start()

        @pl.when(on(n - 1))
        def _():
            for copy in hop_d(n - 1):
                copy.start()

    def compute(n):
        s, g = n % 2, n % n_g

        def one(t, _):
            where = pl.ds(pl.multiple_of(t * tile, tile), tile)
            d_val = d[where, :]
            d_low = d_val.astype(BF16)
            db[where, :] = d_low
            q = jnp.dot(d_low, w2t[s], preferred_element_type=F32)
            r_val = (p[s, where, :] * q).astype(BF16)
            r[where, :] = r_val

            @pl.when(n < layers - 1)
            def _():
                d[where, :] = d_val + jnp.dot(r_val, w1t[s], preferred_element_type=F32)

            return 0

        lax.fori_loop(0, tiles, one, 0)

        def out_grad(m, _):
            val = jnp.dot(zt[s, pl.ds(pl.multiple_of(m * 4 * s2, 4 * s2), 4 * s2), :], db[...], preferred_element_type=F32)
            val = val.astype(BF16)
            for k in range(4):
                gb[g, k % 2, k // 2, m] = val[k * s2:(k + 1) * s2]
            return 0

        def in_grad(m, _):
            val = jnp.dot(at[s, pl.ds(pl.multiple_of(m * 4 * s1, 4 * s1), 4 * s1), :], r[...], preferred_element_type=F32)
            val = val.astype(BF16)
            for k in range(4):
                ga[g, k % 2, m, k // 2] = val[k * s1:(k + 1) * s1]
            return 0

        lax.fori_loop(0, 2, out_grad, 0)
        lax.fori_loop(0, 2, in_grad, 0)

    d_copy = pltpu.make_async_copy(d_in, d, d_sem)
    d_copy.start()
    for copy in loads(0):
        copy.start()
    d_copy.wait()

    def turn(n, _):
        exchange(n)

        @pl.when(n < layers)
        def _():
            for copy in loads(n):
                copy.wait()

            @pl.when(n + 1 < layers)
            def _():
                for copy in loads(n + 1):
                    copy.start()

            compute(n)

        return 0

    lax.fori_loop(0, layers + lag_4, turn, 0)
    for n in (layers - 2, layers - 1):
        for copy in results(n):
            copy.wait()


def backward(d0, zt, at, p, w1t, w2t, n_dev, tile=512, cid=1):
    layers, d_ff, rows = zt.shape
    d_model = d0.shape[1]
    s1, s2 = d_model // n_dev, d_ff // n_dev
    sds = jax.ShapeDtypeStruct
    vm, sem = pltpu.VMEM, pltpu.SemaphoreType.DMA
    n_g, n_d, n_r1, n_s, n_r2, n_t = 2, 2 * WAIT_D, 2 * WAIT_1, WAIT_1 + 1, 2 * WAIT_2, WAIT_2 + 1
    scratch = [
        vm((rows, d_model), F32), vm((rows, d_model), BF16), vm((rows, d_ff), BF16),
        vm((2, d_ff, rows), BF16), vm((2, d_model, rows), BF16), vm((2, rows, d_ff), F32),
        vm((2, d_ff, d_model), BF16), vm((2, d_model, d_ff), BF16),
        vm((n_g, 2, 2, 2, s1, d_ff), BF16), vm((n_g, 2, 2, 2, s2, d_model), BF16),
        vm((n_d, 2, 2, s1, d_ff), BF16), vm((n_d, 2, 2, s2, d_model), BF16),
        vm((n_s, 2, 2, s1, d_ff), BF16), vm((n_s, 2, 2, s2, d_model), BF16),
        vm((n_r1, 2, s1, d_ff), BF16), vm((n_r1, 2, s2, d_model), BF16),
        vm((n_t, 2, s1, d_ff), BF16), vm((n_t, 2, s2, d_model), BF16),
        vm((n_r2, s1, d_ff), BF16), vm((n_r2, s2, d_model), BF16),
        vm((2, s1, d_ff), BF16), vm((2, s2, d_model), BF16),
        sem((2, 5)), sem(()), sem((n_d, 2)), sem((n_d, 2)), sem((n_r1, 2)), sem((n_r1, 2)),
        sem((n_r2, 2)), sem((n_r2, 2)), sem((2, 2)),
    ]
    return pl.pallas_call(
        functools.partial(backward_kernel, layers, tile),
        out_shape=(sds((layers, s1, d_ff), BF16), sds((layers, s2, d_model), BF16)),
        in_specs=[ANY] * 6,
        out_specs=(ANY, ANY),
        scratch_shapes=scratch,
        compiler_params=pltpu.CompilerParams(collective_id=cid, has_side_effects=True, vmem_limit_bytes=63 * 2**20),
        name="bwd",
    )(d0, zt, at, p, w1t, w2t)


def solution(mesh):
    n_dev = mesh.shape["data"]
    w_spec = P(None, "data", None)
    row_spec = P("data", None)

    def device_step(w_one, w_two, mom_one, mom_two, x_zero, y_zero, x_one, y_one):
        tok_dev, d_model = x_zero.shape
        scale = float(n_dev * tok_dev * d_model)
        d0, zt, at, p, w1t, w2t = forward(True, w_one.astype(BF16), w_two.astype(BF16), x_zero, y_zero, scale, cid=0)
        g1, g2 = backward(d0, zt, at, p, w1t, w2t, n_dev, cid=1)
        new_mom_one = MOMENTUM * mom_one + g1.astype(F32)
        new_mom_two = MOMENTUM * mom_two + g2.astype(F32)
        new_w_one = w_one - LEARN_RATE * new_mom_one
        new_w_two = w_two - LEARN_RATE * new_mom_two
        h_last = forward(False, new_w_one.astype(BF16), new_w_two.astype(BF16), x_one, cid=2)
        loss_rows = jnp.sum(jnp.square(h_last - y_one.astype(F32)), axis=1) / (2 * d_model)
        return new_w_one, new_w_two, new_mom_one, new_mom_two, loss_rows, h_last

    return jax.shard_map(device_step, mesh=mesh, in_specs=(w_spec, w_spec, w_spec, w_spec, row_spec, row_spec, row_spec, row_spec), out_specs=(w_spec, w_spec, w_spec, w_spec, P("data"), row_spec), check_vma=False)
```

```python
import functools

import jax
import jax.numpy as jnp
from jax import lax
from jax.experimental import pallas as pl
from jax.experimental.pallas import tpu as pltpu
from jax.sharding import PartitionSpec as P

LEARN_RATE = 0.1
MOMENTUM = 0.9
GELU_C = 0.7978845608028654
GELU_K = 0.044715
MESH = pl.DeviceIdType.MESH
F32 = jnp.float32
BF16 = jnp.bfloat16
AHEAD_CORE, AHEAD_RELAY, AHEAD_OWN = 1, 2, 4
SLOTS = AHEAD_OWN + 2
CHUNK = 512
ANY = pl.BlockSpec(memory_space=pl.ANY)


def place():
    me = lax.axis_index("data")
    core, col, row = me % 2, (me // 2) % 2, me // 4
    return me, core, col, row


def index_of(row, col, core):
    return 4 * row + 2 * col + core


def greet(peers):
    barrier = pltpu.get_barrier_semaphore()
    for peer in peers:
        pl.semaphore_signal(barrier, inc=1, device_id=(peer,), device_id_type=MESH)
    pl.semaphore_wait(barrier, len(peers))


def forward_kernel(train, layers, tile, scale, *refs):
    if train:
        (w1s, w2s, x_in, y_in, d_out, zt_out, at_out, p_out, w1t_out, w2t_out,
         w1, w2, h, xb, s1_st, s2_st, send_sem, recv_sem, own_sem, io_sem,
         zt_st, at_st, p_st, w1t_st, w2t_st, st_sem, wt_sem) = refs
    else:
        (w1s, w2s, x_in, h_out, w1, w2, h, xb, s1_st, s2_st, send_sem, recv_sem, own_sem, io_sem) = refs
    me, core, col, row = place()
    j_p = index_of(row, col, 1 - core)
    j_x = index_of(row, 1 - col, core)
    j_y = index_of(1 - row, col, core)
    j_d = index_of(1 - row, 1 - col, core)
    p_x = index_of(row, 1 - col, 1 - core)
    p_y = index_of(1 - row, col, 1 - core)
    p_d = index_of(1 - row, 1 - col, 1 - core)
    r1, r2 = w1s.shape[1], w2s.shape[1]
    rows = h.shape[0]
    tiles = rows // tile

    greet((j_p, j_x, j_y))

    def part(which, slot, j):
        if which == 1:
            return w1.at[slot, pl.ds(pl.multiple_of(j * r1, r1), r1)]
        return w2.at[slot, pl.ds(pl.multiple_of(j * r2, r2), r2)]

    sends = (
        (1, me, j_y, j_y), (1, me, j_x, j_x), (1, me, j_p, j_p),
        (2, me, j_x, j_x), (2, me, j_y, j_y), (2, me, j_p, j_p),
        (1, j_y, j_x, j_d), (1, j_y, j_p, p_y), (2, j_x, j_y, j_d), (2, j_x, j_p, p_x),
        (1, j_x, j_p, p_x), (2, j_y, j_p, p_y),
        (1, j_d, j_p, p_d), (2, j_d, j_p, p_d),
    )

    def channel(layer, k, incoming=False):
        slot = layer % SLOTS
        which, out, to, inc = sends[k]
        ref = part(which, slot, inc if incoming else out)
        return pltpu.make_async_remote_copy(
            src_ref=ref, dst_ref=ref, send_sem=send_sem.at[slot, k], recv_sem=recv_sem.at[slot, k],
            device_id=(to,), device_id_type=MESH)

    def start(layer, ks):
        for k in ks:
            channel(layer, k).start()

    def arrive(layer, ks):
        for k in ks:
            channel(layer, k, True).wait_recv()

    def own(layer):
        st = layer % 2
        return (pltpu.make_async_copy(w1s.at[layer], s1_st.at[st], own_sem.at[st, 0]),
                pltpu.make_async_copy(w2s.at[layer], s2_st.at[st], own_sem.at[st, 1]))

    def place_own(layer):
        for copy in own(layer):
            copy.wait()
        part(1, layer % SLOTS, me)[...] = s1_st[layer % 2].astype(BF16)
        part(2, layer % SLOTS, me)[...] = s2_st[layer % 2].astype(BF16)

    def on(layer):
        return jnp.logical_and(layer >= 0, layer < layers)

    def gather(i):
        @pl.when(on(i + AHEAD_CORE))
        def _():
            arrive(i + AHEAD_CORE, (6, 8))
            start(i + AHEAD_CORE, (12, 13))

        @pl.when(on(i + AHEAD_RELAY))
        def _():
            arrive(i + AHEAD_RELAY, (0, 1, 3, 4))
            start(i + AHEAD_RELAY, (6, 8, 7, 9, 10, 11))

        @pl.when(on(i + AHEAD_OWN))
        def _():
            place_own(i + AHEAD_OWN)
            start(i + AHEAD_OWN, (0, 3, 1, 4, 2, 5))

        @pl.when(on(i + AHEAD_OWN + 2))
        def _():
            for copy in own(i + AHEAD_OWN + 2):
                copy.start()

    def saved(layer, t, st):
        cols = pl.ds(pl.multiple_of(t * tile, tile), tile)
        return (pltpu.make_async_copy(zt_st.at[st], zt_out.at[layer, :, cols], st_sem.at[st, 0]),
                pltpu.make_async_copy(at_st.at[st], at_out.at[layer, :, cols], st_sem.at[st, 1]),
                pltpu.make_async_copy(p_st.at[st], p_out.at[layer, cols], st_sem.at[st, 2]))

    def turned(layer):
        return (pltpu.make_async_copy(w1t_st, w1t_out.at[layer], wt_sem.at[0]),
                pltpu.make_async_copy(w2t_st, w2t_out.at[layer], wt_sem.at[1]))

    def compute(layer):
        slot = layer % SLOTS

        def one(t):
            where = pl.ds(t * tile, tile)
            h_val = h[where, :]
            a_val = h_val.astype(BF16)
            step = layer * tiles + t
            st = step % 2
            if train:
                @pl.when(step >= 2)
                def _():
                    for copy in saved((step - 2) // tiles, (step - 2) % tiles, st):
                        copy.wait()

                at_st[st] = a_val.T
            lows = []
            for c in range(0, w1.shape[2], CHUNK):
                cut = slice(c, c + CHUNK)
                u = jnp.dot(a_val, w1[slot, :, cut], preferred_element_type=F32)
                sq = u * u
                w = 0.5 * (1.0 + jnp.tanh(u * (GELU_C + (GELU_C * GELU_K) * sq)))
                z = u * w
                z_low = z.astype(BF16)
                lows.append(z_low)
                if train:
                    p_st[st, :, cut] = w + (z * (1.0 - w)) * (2.0 * GELU_C + (6.0 * GELU_C * GELU_K) * sq)
                    zt_st[st, cut, :] = z_low.T
            if train:
                for copy in saved(layer, t, st):
                    copy.start()
            z_low = jnp.concatenate(lows, axis=1)
            h[where, :] = h_val + jnp.dot(z_low, w2[slot], preferred_element_type=F32)

        one(0)
        gather(layer)
        for t in range(1, tiles):
            one(t)
        if train:
            @pl.when(layer >= 1)
            def _():
                for copy in turned(layer - 1):
                    copy.wait()

            w1t_st[...] = w1[slot].T
            w2t_st[...] = w2[slot].T
            for copy in turned(layer):
                copy.start()

    x_copy = pltpu.make_async_copy(x_in, xb, io_sem.at[0])
    x_copy.start()
    for layer in (0, 1):
        for copy in own(layer):
            copy.start()

    def widen(t, _):
        where = pl.ds(pl.multiple_of(t * 256, 256), 256)
        h[where, :] = xb[where, :].astype(F32)
        return 0

    def turn(n, _):
        i = n - AHEAD_OWN

        @pl.when(i < 0)
        def _():
            gather(i)

        @pl.when(i == -1)
        def _():
            x_copy.wait()
            lax.fori_loop(0, rows // 256, widen, 0)

        @pl.when(i >= 0)
        def _():
            arrive(i, (2, 5, 7, 9, 10, 11, 12, 13))
            compute(i)
            for k in range(len(sends)):
                channel(i, k).wait_send()

        return 0

    lax.fori_loop(0, layers + AHEAD_OWN, turn, 0)

    if train:
        last = layers * tiles
        for step in (last - 2, last - 1):
            for copy in saved(step // tiles, step % tiles, step % 2):
                copy.wait()
        for copy in turned(layers - 1):
            copy.wait()
        y_copy = pltpu.make_async_copy(y_in, xb, io_sem.at[0])
        y_copy.start()
        y_copy.wait()

        def close(t, _):
            where = pl.ds(pl.multiple_of(t * 256, 256), 256)
            h[where, :] = (h[where, :] - xb[where, :].astype(F32)) / scale
            return 0

        lax.fori_loop(0, rows // 256, close, 0)
    out_copy = pltpu.make_async_copy(h, d_out if train else h_out, io_sem.at[1])
    out_copy.start()
    out_copy.wait()


def forward(train, w1s, w2s, x, y=None, scale=None, tile=768, cid=0):
    layers, r1, d_ff = w1s.shape
    r2, d_model = w2s.shape[1:]
    rows = x.shape[0]
    sds = jax.ShapeDtypeStruct
    h_shape = sds((rows, d_model), F32)
    scratch = [
        pltpu.VMEM((SLOTS, d_model, d_ff), BF16), pltpu.VMEM((SLOTS, d_ff, d_model), BF16),
        pltpu.VMEM((rows, d_model), F32), pltpu.VMEM((rows, d_model), BF16),
        pltpu.VMEM((2, r1, d_ff), F32), pltpu.VMEM((2, r2, d_model), F32),
        pltpu.SemaphoreType.DMA((SLOTS, 14)), pltpu.SemaphoreType.DMA((SLOTS, 14)),
        pltpu.SemaphoreType.DMA((2, 2)), pltpu.SemaphoreType.DMA((2,)),
    ]
    out = h_shape
    args = (w1s, w2s, x)
    if train:
        out = (h_shape, sds((layers, d_ff, rows), BF16), sds((layers, d_model, rows), BF16),
               sds((layers, rows, d_ff), F32), sds((layers, d_ff, d_model), BF16), sds((layers, d_model, d_ff), BF16))
        args = (w1s, w2s, x, y)
        scratch += [
            pltpu.VMEM((2, d_ff, tile), BF16), pltpu.VMEM((2, d_model, tile), BF16), pltpu.VMEM((2, tile, d_ff), F32),
            pltpu.VMEM((d_ff, d_model), BF16), pltpu.VMEM((d_model, d_ff), BF16),
            pltpu.SemaphoreType.DMA((2, 3)), pltpu.SemaphoreType.DMA((2,)),
        ]
    return pl.pallas_call(
        functools.partial(forward_kernel, train, layers, tile, scale),
        out_shape=out,
        in_specs=[ANY] * len(args),
        out_specs=jax.tree.map(lambda _: ANY, out),
        scratch_shapes=scratch,
        compiler_params=pltpu.CompilerParams(collective_id=cid, has_side_effects=True, vmem_limit_bytes=60 * 2**20),
        name="fwd_train" if train else "fwd_eval",
    )(*args)


def backward_kernel(layers, *refs):
    (d_in, zt_in, at_in, p_in, w1t_in, w2t_in, g1_out, g2_out,
     d, db, r, zt, at, p, w1t, w2t, ga, gb, da, dbuf, sa, sb, ra, rb, ta, tb, fa, fb, oa, ob,
     in_sem, d_sem, xd_send, xd_recv, x1_send, x1_recv, x2_send, x2_recv, out_sem) = refs
    me, core, col, row = place()
    j_p = index_of(row, col, 1 - core)
    j_x = index_of(row, 1 - col, core)
    j_y = index_of(1 - row, col, core)
    n_d, n_r = da.shape[0], ra.shape[0]
    s1, s2 = ga.shape[4], gb.shape[4]

    greet((j_p, j_x, j_y))

    def loads(n):
        layer, s = layers - 1 - n, n % 2
        return tuple(
            pltpu.make_async_copy(src.at[layer], dst.at[s], in_sem.at[s, k])
            for k, (src, dst) in enumerate(((w2t_in, w2t), (p_in, p), (w1t_in, w1t), (zt_in, zt), (at_in, at))))

    def remote(src, dst, send, recv, to):
        return pltpu.make_async_remote_copy(
            src_ref=src, dst_ref=dst, send_sem=send, recv_sem=recv, device_id=(to,), device_id_type=MESH)

    def hop_d(n, k):
        g, s = n % 2, n % n_d
        src, dst = ((ga, da), (gb, dbuf))[k]
        return remote(src.at[g, 1 - core], dst.at[s], xd_send.at[s, k], xd_recv.at[s, k], j_p)

    def hop_1(n, k):
        g, s = n % 2, n % n_r
        src, dst, away, to = ((sa, ra, 1 - row, j_y), (sb, rb, 1 - col, j_x))[k]
        return remote(src.at[g, away], dst.at[s], x1_send.at[s, k], x1_recv.at[s, k], to)

    def hop_2(n, k):
        g, s = n % 2, n % n_r
        src, dst, away, to = ((ta, fa, 1 - col, j_x), (tb, fb, 1 - row, j_y))[k]
        return remote(src.at[g, away], dst.at[s], x2_send.at[s, k], x2_recv.at[s, k], to)

    def result(n, k):
        s = n % 2
        src, dst = ((oa, g1_out), (ob, g2_out))[k]
        return pltpu.make_async_copy(src.at[s], dst.at[layers - 1 - n], out_sem.at[s, k])

    def on(n):
        return jnp.logical_and(n >= 0, n < layers)

    def add(x, y):
        return (x.astype(F32) + y.astype(F32)).astype(BF16)

    def sum_core(m, k):
        @pl.when(on(m))
        def _():
            hop_d(m, k).wait()
            src, got, out = ((ga, da, sa), (gb, dbuf, sb))[k]
            out[m % 2] = add(src[m % 2, core], got[m % n_d])
            hop_1(m, k).start()

    def sum_first(m, k):
        @pl.when(on(m))
        def _():
            hop_1(m, k).wait()
            src, got, out, here = ((sa, ra, ta, row), (sb, rb, tb, col))[k]
            out[m % 2] = add(src[m % 2, here], got[m % n_r])
            hop_2(m, k).start()

    def sum_second(m, k):
        @pl.when(on(m))
        def _():
            @pl.when(m >= 2)
            def _():
                result(m - 2, k).wait()

            hop_2(m, k).wait()
            src, got, out, here = ((ta, fa, oa, col), (tb, fb, ob, row))[k]
            out[m % 2] = add(src[m % 2, here], got[m % n_r])
            result(m, k).start()

    def early(n):
        sum_second(n - 3, 1)
        sum_first(n - 2, 1)
        sum_core(n - 1, 0)

    def late(n):
        sum_second(n - 3, 0)
        sum_first(n - 2, 0)
        sum_core(n, 1)

    def out_grad(n):
        s, g = n % 2, n % 2
        db[...] = d[...].astype(BF16)
        val = jnp.dot(zt[s], db[...], preferred_element_type=F32).astype(BF16)
        for k in range(8):
            gb[g, k % 2, (k // 2) % 2, k // 4] = val[k * s2:(k + 1) * s2]

    def in_back(n):
        s = n % 2
        q = jnp.dot(db[...], w2t[s], preferred_element_type=F32)
        r[...] = (p[s] * q).astype(BF16)

        @pl.when(n < layers - 1)
        def _():
            d[...] = d[...] + jnp.dot(r[...], w1t[s], preferred_element_type=F32)

    def in_grad(n):
        s, g = n % 2, n % 2
        val = jnp.dot(at[s], r[...], preferred_element_type=F32).astype(BF16)
        for k in range(8):
            ga[g, k % 2, k // 4, (k // 2) % 2] = val[k * s1:(k + 1) * s1]

    d_copy = pltpu.make_async_copy(d_in, d, d_sem)
    d_copy.start()
    for copy in loads(0):
        copy.start()
    d_copy.wait()

    def turn(n, _):
        @pl.when(n < layers)
        def _():
            for copy in loads(n):
                copy.wait()

            @pl.when(n + 1 < layers)
            def _():
                for copy in loads(n + 1):
                    copy.start()

            out_grad(n)

        early(n)

        @pl.when(n < layers)
        def _():
            hop_d(n, 1).start()
            in_back(n)

        late(n)

        @pl.when(n < layers)
        def _():
            in_grad(n)
            hop_d(n, 0).start()

        return 0

    lax.fori_loop(0, layers + 3, turn, 0)
    for n in (layers - 2, layers - 1):
        for k in range(2):
            result(n, k).wait()


def backward(d0, zt, at, p, w1t, w2t, n_dev, cid=1):
    layers, d_ff, rows = zt.shape
    d_model = d0.shape[1]
    s1, s2 = d_model // n_dev, d_ff // n_dev
    sds = jax.ShapeDtypeStruct
    vm, sem = pltpu.VMEM, pltpu.SemaphoreType.DMA
    n_d, n_r = 2, 4
    scratch = [
        vm((rows, d_model), F32), vm((rows, d_model), BF16), vm((rows, d_ff), BF16),
        vm((2, d_ff, rows), BF16), vm((2, d_model, rows), BF16), vm((2, rows, d_ff), F32),
        vm((2, d_ff, d_model), BF16), vm((2, d_model, d_ff), BF16),
        vm((2, 2, 2, 2, s1, d_ff), BF16), vm((2, 2, 2, 2, s2, d_model), BF16),
        vm((n_d, 2, 2, s1, d_ff), BF16), vm((n_d, 2, 2, s2, d_model), BF16),
        vm((2, 2, 2, s1, d_ff), BF16), vm((2, 2, 2, s2, d_model), BF16),
        vm((n_r, 2, s1, d_ff), BF16), vm((n_r, 2, s2, d_model), BF16),
        vm((2, 2, s1, d_ff), BF16), vm((2, 2, s2, d_model), BF16),
        vm((n_r, s1, d_ff), BF16), vm((n_r, s2, d_model), BF16),
        vm((2, s1, d_ff), BF16), vm((2, s2, d_model), BF16),
        sem((2, 5)), sem(()), sem((n_d, 2)), sem((n_d, 2)), sem((n_r, 2)), sem((n_r, 2)),
        sem((n_r, 2)), sem((n_r, 2)), sem((2, 2)),
    ]
    return pl.pallas_call(
        functools.partial(backward_kernel, layers),
        out_shape=(sds((layers, s1, d_ff), BF16), sds((layers, s2, d_model), BF16)),
        in_specs=[ANY] * 6,
        out_specs=(ANY, ANY),
        scratch_shapes=scratch,
        compiler_params=pltpu.CompilerParams(collective_id=cid, has_side_effects=True, vmem_limit_bytes=63 * 2**20),
        name="bwd",
    )(d0, zt, at, p, w1t, w2t)


def solution(mesh):
    n_dev = mesh.shape["data"]
    w_spec = P(None, "data", None)
    row_spec = P("data", None)

    def device_step(w_one, w_two, mom_one, mom_two, x_zero, y_zero, x_one, y_one):
        tok_dev, d_model = x_zero.shape
        scale = float(n_dev * tok_dev * d_model)
        d0, zt, at, p, w1t, w2t = forward(True, w_one, w_two, x_zero, y_zero, scale, cid=0)
        g1, g2 = backward(d0, zt, at, p, w1t, w2t, n_dev, cid=1)
        new_mom_one = MOMENTUM * mom_one + g1.astype(F32)
        new_mom_two = MOMENTUM * mom_two + g2.astype(F32)
        new_w_one = w_one - LEARN_RATE * new_mom_one
        new_w_two = w_two - LEARN_RATE * new_mom_two
        h_last = forward(False, new_w_one, new_w_two, x_one, cid=2)
        loss_rows = jnp.sum(jnp.square(h_last - y_one.astype(F32)), axis=1) / (2 * d_model)
        return new_w_one, new_w_two, new_mom_one, new_mom_two, loss_rows, h_last

    return jax.shard_map(device_step, mesh=mesh, in_specs=(w_spec, w_spec, w_spec, w_spec, row_spec, row_spec, row_spec, row_spec), out_specs=(w_spec, w_spec, w_spec, w_spec, P("data"), row_spec), check_vma=False)
```

```python
import functools

import jax
import jax.numpy as jnp
from jax import lax
from jax.experimental import pallas as pl
from jax.experimental.pallas import tpu as pltpu
from jax.sharding import PartitionSpec as P

LEARN_RATE = 0.1
MOMENTUM = 0.9
GELU_C = 0.7978845608028654
GELU_K = 0.044715
MESH = pl.DeviceIdType.MESH
F32 = jnp.float32
BF16 = jnp.bfloat16
AHEAD_CORE, AHEAD_RELAY = 1, 2
PRE = 5
CHUNK = 512
FIRST = (0, 3, 1, 4)
ANY = pl.BlockSpec(memory_space=pl.ANY)


def place():
    me = lax.axis_index("data")
    core, col, row = me % 2, (me // 2) % 2, me // 4
    return me, core, col, row


def index_of(row, col, core):
    return 4 * row + 2 * col + core


def greet(peers):
    barrier = pltpu.get_barrier_semaphore()
    for peer in peers:
        pl.semaphore_signal(barrier, inc=1, device_id=(peer,), device_id_type=MESH)
    return lambda: pl.semaphore_wait(barrier, len(peers))


def forward_kernel(train, layers, tile, scale, ahead, *refs):
    pre, slots = 0 if train else PRE, ahead + 2
    eager = 0 if train else 2
    if train:
        (w1s, w2s, x_in, y_in, d_out, zt_out, at_out, p_out, w1t_out, w2t_out,
         w1, w2, h, xb, s1_st, s2_st, send_sem, recv_sem, own_sem, io_sem, out_sem,
         zt_st, at_st, p_st, w1t_st, w2t_st, st_sem, wt_sem) = refs
    else:
        (w1s, w2s, x_in, xs, ys, h_out, w1, w2, h, xb, s1_st, s2_st, send_sem, recv_sem, own_sem, io_sem, out_sem, pre_sem) = refs
    me, core, col, row = place()
    j_p = index_of(row, col, 1 - core)
    j_x = index_of(row, 1 - col, core)
    j_y = index_of(1 - row, col, core)
    j_d = index_of(1 - row, 1 - col, core)
    p_x = index_of(row, 1 - col, 1 - core)
    p_y = index_of(1 - row, col, 1 - core)
    p_d = index_of(1 - row, 1 - col, 1 - core)
    r1, r2 = w1s.shape[1], w2s.shape[1]
    rows = h.shape[0]
    tiles = rows // tile

    met = greet((j_p, j_x, j_y))

    def part(which, slot, j):
        if which == 1:
            return w1.at[slot, pl.ds(pl.multiple_of(j * r1, r1), r1)]
        return w2.at[slot, pl.ds(pl.multiple_of(j * r2, r2), r2)]

    sends = (
        (1, me, j_y, j_y), (1, me, j_x, j_x), (1, me, j_p, j_p),
        (2, me, j_x, j_x), (2, me, j_y, j_y), (2, me, j_p, j_p),
        (1, j_y, j_x, j_d), (1, j_y, j_p, p_y), (2, j_x, j_y, j_d), (2, j_x, j_p, p_x),
        (1, j_x, j_p, p_x), (2, j_y, j_p, p_y),
        (1, j_d, j_p, p_d), (2, j_d, j_p, p_d),
    )

    def channel(layer, k, incoming=False):
        slot = layer % slots
        which, out, to, inc = sends[k]
        ref = part(which, slot, inc if incoming else out)
        return pltpu.make_async_remote_copy(
            src_ref=ref, dst_ref=ref, send_sem=send_sem.at[slot, k], recv_sem=recv_sem.at[slot, k],
            device_id=(to,), device_id_type=MESH)

    def start(layer, ks):
        for k in ks:
            channel(layer, k).start()

    def arrive(layer, ks):
        for k in ks:
            channel(layer, k, True).wait_recv()

    def own(layer):
        st = layer % 2
        return (pltpu.make_async_copy(w1s.at[layer], s1_st.at[st], own_sem.at[st, 0]),
                pltpu.make_async_copy(w2s.at[layer], s2_st.at[st], own_sem.at[st, 1]))

    def given(layer):
        slot, half = layer % slots, w2.shape[2]
        copies = []
        for src, j in ((xs, j_x), (ys, j_y)):
            copies.append((src.at[layer, 0], part(1, slot, j)))
            for i in range(2):
                rows_2 = pl.ds(pl.multiple_of(j * r2 + i * r1, r1), r1)
                copies.append((src.at[layer, 1, :, pl.ds(i * half, half)], w2.at[slot, rows_2]))
        return tuple(pltpu.make_async_copy(src, dst, pre_sem.at[layer, k]) for k, (src, dst) in enumerate(copies))

    def place_own(layer):
        for copy in own(layer):
            copy.wait()
        part(1, layer % slots, me)[...] = s1_st[layer % 2].astype(BF16)
        part(2, layer % slots, me)[...] = s2_st[layer % 2].astype(BF16)

    def leave(layer):
        place_own(layer)

        @pl.when(layer >= pre)
        def _():
            start(layer, FIRST)

        start(layer, (2, 5))

    def relay(layer):
        if pre:
            @pl.when(layer < pre)
            def _():
                for copy in given(layer):
                    copy.wait()

        @pl.when(layer >= pre)
        def _():
            arrive(layer, FIRST)

        start(layer, (6, 8, 7, 9, 10, 11))

    def on(layer):
        return jnp.logical_and(layer >= 0, layer < layers)

    def gather(i):
        @pl.when(on(i + AHEAD_CORE))
        def _():
            arrive(i + AHEAD_CORE, (6, 8))
            start(i + AHEAD_CORE, (12, 13))

        @pl.when(jnp.logical_and(on(i + AHEAD_RELAY), i + AHEAD_RELAY >= eager))
        def _():
            relay(i + AHEAD_RELAY)

        @pl.when(on(i + ahead))
        def _():
            leave(i + ahead)

        @pl.when(on(i + ahead + 2))
        def _():
            for copy in own(i + ahead + 2):
                copy.start()

    def saved(layer, t, st):
        cols = pl.ds(pl.multiple_of(t * tile, tile), tile)
        return (pltpu.make_async_copy(zt_st.at[st], zt_out.at[layer, :, cols], st_sem.at[st, 0]),
                pltpu.make_async_copy(at_st.at[st], at_out.at[layer, :, cols], st_sem.at[st, 1]),
                pltpu.make_async_copy(p_st.at[st], p_out.at[layer, cols], st_sem.at[st, 2]))

    def final(t):
        where = pl.ds(t * tile, tile)
        return pltpu.make_async_copy(h.at[where], (d_out if train else h_out).at[where], out_sem.at[t])

    def turned(layer):
        return (pltpu.make_async_copy(w1t_st, w1t_out.at[layer], wt_sem.at[0]),
                pltpu.make_async_copy(w2t_st, w2t_out.at[layer], wt_sem.at[1]))

    def compute(layer):
        slot = layer % slots

        def one(t):
            where = pl.ds(t * tile, tile)
            h_val = h[where, :]
            a_val = h_val.astype(BF16)
            step = layer * tiles + t
            st = step % 2
            if train:
                @pl.when(step >= 2)
                def _():
                    for copy in saved((step - 2) // tiles, (step - 2) % tiles, st):
                        copy.wait()

                at_st[st] = a_val.T
            lows = []
            for c in range(0, w1.shape[2], CHUNK):
                cut = slice(c, c + CHUNK)
                u = jnp.dot(a_val, w1[slot, :, cut], preferred_element_type=F32)
                sq = u * u
                w = 0.5 * (1.0 + jnp.tanh(u * (GELU_C + (GELU_C * GELU_K) * sq)))
                z = u * w
                z_low = z.astype(BF16)
                lows.append(z_low)
                if train:
                    p_st[st, :, cut] = w + (z * (1.0 - w)) * (2.0 * GELU_C + (6.0 * GELU_C * GELU_K) * sq)
                    zt_st[st, cut, :] = z_low.T
            if train:
                for copy in saved(layer, t, st):
                    copy.start()
            z_low = jnp.concatenate(lows, axis=1)
            h[where, :] = h_val + jnp.dot(z_low, w2[slot], preferred_element_type=F32)

            @pl.when(layer == layers - 1)
            def _():
                if train:
                    if t == 0:
                        y_copy.wait()
                    h[where, :] = (h[where, :] - xb[where, :].astype(F32)) / scale
                final(t).start()

        one(0)
        gather(layer)
        for t in range(1, tiles):
            one(t)
        if train:
            @pl.when(layer >= 1)
            def _():
                for copy in turned(layer - 1):
                    copy.wait()

            w1t_st[...] = w1[slot].T
            w2t_st[...] = w2[slot].T
            for copy in turned(layer):
                copy.start()

    x_copy = pltpu.make_async_copy(x_in, xb, io_sem.at[0])
    if train:
        y_copy = pltpu.make_async_copy(y_in, xb, io_sem.at[1])
    x_copy.start()
    for layer in (0, 1):
        for copy in own(layer):
            copy.start()
    for layer in range(pre):
        for copy in given(layer):
            copy.start()
    met()

    def widen(t, _):
        where = pl.ds(pl.multiple_of(t * 256, 256), 256)
        h[where, :] = xb[where, :].astype(F32)
        return 0

    def turn(n, _):
        i = n - ahead

        @pl.when(i < 0)
        def _():
            gather(i)

        @pl.when(i == -1)
        def _():
            x_copy.wait()
            lax.fori_loop(0, rows // 256, widen, 0)
            if train:
                y_copy.start()

        @pl.when(i >= 0)
        def _():
            arrive(i, (2, 5, 7, 9, 10, 11, 12, 13))
            compute(i)
            for k in range(len(sends)):
                if pre and k in FIRST:
                    @pl.when(i >= pre)
                    def _(k=k):
                        channel(i, k).wait_send()
                else:
                    channel(i, k).wait_send()

        return 0

    if not train:
        for layer in range(ahead - 1):
            leave(jnp.int32(layer))
            for copy in own(layer + 2):
                copy.start()
            if layer < eager:
                relay(jnp.int32(layer))
    lax.fori_loop(0 if train else ahead - 1, layers + ahead, turn, 0)

    if train:
        last = layers * tiles
        for step in (last - 2, last - 1):
            for copy in saved(step // tiles, step % tiles, step % 2):
                copy.wait()
        for copy in turned(layers - 1):
            copy.wait()
    for t in range(tiles):
        final(t).wait()


def forward(train, w1s, w2s, x, *more, scale=None, tile=768, ahead=4, cid=0):
    slots = ahead + 2
    layers, r1, d_ff = w1s.shape
    r2, d_model = w2s.shape[1:]
    rows = x.shape[0]
    sds = jax.ShapeDtypeStruct
    h_shape = sds((rows, d_model), F32)
    scratch = [
        pltpu.VMEM((slots, d_model, d_ff), BF16), pltpu.VMEM((slots, d_ff, d_model), BF16),
        pltpu.VMEM((rows, d_model), F32), pltpu.VMEM((rows, d_model), BF16),
        pltpu.VMEM((2, r1, d_ff), w1s.dtype), pltpu.VMEM((2, r2, d_model), w2s.dtype),
        pltpu.SemaphoreType.DMA((slots, 14)), pltpu.SemaphoreType.DMA((slots, 14)),
        pltpu.SemaphoreType.DMA((2, 2)), pltpu.SemaphoreType.DMA((2,)), pltpu.SemaphoreType.DMA((rows // tile,)),
    ]
    out = h_shape
    args = (w1s, w2s, x, *more)
    if not train:
        scratch += [pltpu.SemaphoreType.DMA((PRE, 6))]
    if train:
        out = (h_shape, sds((layers, d_ff, rows), BF16), sds((layers, d_model, rows), BF16),
               sds((layers, rows, d_ff), F32), sds((layers, d_ff, d_model), BF16), sds((layers, d_model, d_ff), BF16))
        scratch += [
            pltpu.VMEM((2, d_ff, tile), BF16), pltpu.VMEM((2, d_model, tile), BF16), pltpu.VMEM((2, tile, d_ff), F32),
            pltpu.VMEM((d_ff, d_model), BF16), pltpu.VMEM((d_model, d_ff), BF16),
            pltpu.SemaphoreType.DMA((2, 3)), pltpu.SemaphoreType.DMA((2,)),
        ]
    return pl.pallas_call(
        functools.partial(forward_kernel, train, layers, tile, scale, ahead),
        out_shape=out,
        in_specs=[ANY] * len(args),
        out_specs=jax.tree.map(lambda _: ANY, out),
        scratch_shapes=scratch,
        compiler_params=pltpu.CompilerParams(collective_id=cid, has_side_effects=True, vmem_limit_bytes=60 * 2**20),
        name="fwd_train" if train else "fwd_eval",
    )(*args)


def backward_kernel(layers, *refs):
    (d_in, zt_in, at_in, p_in, w1t_in, w2t_in, w1s, w2s, m1s, m2s, g1_out, g2_out, nw1_out, nw2_out, first_out,
     d, db, r, zt, at, p, w1t, w2t, ga, gb, da, dbuf, sa, sb, ra, rb, ta, tb, fa, fb, oa, ob, na, nb, wa, wb, ma, mb,
     in_sem, own_sem, first_sem, d_sem, xd_send, xd_recv, x1_send, x1_recv, x2_send, x2_recv, out_sem) = refs
    me, core, col, row = place()
    j_p = index_of(row, col, 1 - core)
    j_x = index_of(row, 1 - col, core)
    j_y = index_of(1 - row, col, core)
    n_d, n_r = da.shape[0], ra.shape[0]
    s1, s2 = ga.shape[4], gb.shape[4]

    met = greet((j_p, j_x, j_y))

    def loads(n):
        layer, s = layers - 1 - n, n % 2
        return tuple(
            pltpu.make_async_copy(src.at[layer], dst.at[s], in_sem.at[s, k])
            for k, (src, dst) in enumerate(((zt_in, zt), (w2t_in, w2t), (p_in, p), (at_in, at), (w1t_in, w1t))))

    def remote(src, dst, send, recv, to):
        return pltpu.make_async_remote_copy(
            src_ref=src, dst_ref=dst, send_sem=send, recv_sem=recv, device_id=(to,), device_id_type=MESH)

    def hop_d(n, k):
        g, s = n % 2, n % n_d
        src, dst = ((ga, da), (gb, dbuf))[k]
        return remote(src.at[g, 1 - core], dst.at[s], xd_send.at[s, k], xd_recv.at[s, k], j_p)

    def hop_1(n, k):
        g, s = n % 2, n % n_r
        src, dst, away, to = ((sa, ra, 1 - row, j_y), (sb, rb, 1 - col, j_x))[k]
        return remote(src.at[g, away], dst.at[s], x1_send.at[s, k], x1_recv.at[s, k], to)

    def hop_2(n, k):
        g, s = n % 2, n % n_r
        src, dst, away, to = ((ta, fa, 1 - col, j_x), (tb, fb, 1 - row, j_y))[k]
        return remote(src.at[g, away], dst.at[s], x2_send.at[s, k], x2_recv.at[s, k], to)

    def result(n, k):
        s = n % 2
        pairs = (((oa, g1_out), (na, nw1_out)), ((ob, g2_out), (nb, nw2_out)))[k]
        return tuple(pltpu.make_async_copy(src.at[s], dst.at[layers - 1 - n], out_sem.at[s, k, i])
                     for i, (src, dst) in enumerate(pairs))

    def first(n, k):
        s, dst = n % 2, first_out.at[layers - 1 - n, k]
        if k == 0:
            return (pltpu.make_async_copy(na.at[s], dst, first_sem.at[s, 0]),)
        half = nb.shape[2]
        return tuple(
            pltpu.make_async_copy(nb.at[s, pl.ds(i * s1, s1)], dst.at[:, pl.ds(i * half, half)], first_sem.at[s, 1 + i])
            for i in range(2))

    def own(n, k):
        s = n % 2
        pairs = (((w1s, wa), (m1s, ma)), ((w2s, wb), (m2s, mb)))[k]
        return tuple(pltpu.make_async_copy(src.at[layers - 1 - n], dst.at[s], own_sem.at[s, k, i])
                     for i, (src, dst) in enumerate(pairs))

    def on(n):
        return jnp.logical_and(n >= 0, n < layers)

    def add(x, y):
        return (x.astype(F32) + y.astype(F32)).astype(BF16)

    def sum_core(m, k):
        @pl.when(on(m))
        def _():
            hop_d(m, k).wait()
            src, got, out = ((ga, da, sa), (gb, dbuf, sb))[k]
            out[m % 2] = add(src[m % 2, core], got[m % n_d])
            hop_1(m, k).start()

    def sum_first(m, k):
        @pl.when(on(m))
        def _():
            for copy in own(m, k):
                copy.start()
            hop_1(m, k).wait()
            src, got, out, here = ((sa, ra, ta, row), (sb, rb, tb, col))[k]
            out[m % 2] = add(src[m % 2, here], got[m % n_r])
            hop_2(m, k).start()

    def sum_second(m, k):
        @pl.when(on(m))
        def _():
            @pl.when(m >= 2)
            def _():
                for copy in result(m - 2, k):
                    copy.wait()

            @pl.when(m - 2 >= layers - PRE)
            def _():
                for copy in first(m - 2, k):
                    copy.wait()

            for copy in own(m, k):
                copy.wait()
            hop_2(m, k).wait()
            src, got, out, here = ((ta, fa, oa, col), (tb, fb, ob, row))[k]
            new, w, mom = ((na, wa, ma), (nb, wb, mb))[k]
            grad = add(src[m % 2, here], got[m % n_r])
            out[m % 2] = grad
            new_mom = MOMENTUM * mom[m % 2] + grad.astype(F32)
            new[m % 2] = (w[m % 2] - LEARN_RATE * new_mom).astype(BF16)
            for copy in result(m, k):
                copy.start()

            @pl.when(m >= layers - PRE)
            def _():
                for copy in first(m, k):
                    copy.start()

    def early(n):
        sum_second(n - 3, 1)
        sum_first(n - 2, 1)

    def late(n):
        sum_second(n - 3, 0)
        sum_first(n - 2, 0)
        sum_core(n, 1)

    def out_grad(n):
        s, g = n % 2, n % 2
        db[...] = d[...].astype(BF16)
        val = jnp.dot(zt[s], db[...], preferred_element_type=F32).astype(BF16)
        for k in range(8):
            gb[g, k % 2, (k // 2) % 2, k // 4] = val[k * s2:(k + 1) * s2]

    def in_back(n):
        s = n % 2
        q = jnp.dot(db[...], w2t[s], preferred_element_type=F32)
        r[...] = (p[s] * q).astype(BF16)

    def state_back(n):
        @pl.when(n < layers - 1)
        def _():
            d[...] = d[...] + jnp.dot(r[...], w1t[n % 2], preferred_element_type=F32)

    def in_grad(n):
        s, g = n % 2, n % 2
        val = jnp.dot(at[s], r[...], preferred_element_type=F32).astype(BF16)
        for k in range(8):
            ga[g, k % 2, k // 4, (k // 2) % 2] = val[k * s1:(k + 1) * s1]

    d_copy = pltpu.make_async_copy(d_in, d, d_sem)
    d_copy.start()
    for copy in loads(0):
        copy.start()
    met()
    d_copy.wait()

    def ready(n, ks):
        copies = loads(n)
        for k in ks:
            copies[k].wait()

    def turn(n, _):
        @pl.when(n < layers)
        def _():
            ready(n, (0,))
            out_grad(n)

        early(n)

        @pl.when(n < layers)
        def _():
            hop_d(n, 1).start()

            @pl.when(n + 1 < layers)
            def _():
                for copy in loads(n + 1):
                    copy.start()

            ready(n, (1, 2))
            in_back(n)

        late(n)

        @pl.when(n < layers)
        def _():
            ready(n, (3, 4))
            in_grad(n)
            hop_d(n, 0).start()
            state_back(n)

        sum_core(n, 0)
        return 0

    lax.fori_loop(0, layers + 3, turn, 0)
    for n in (layers - 2, layers - 1):
        for k in range(2):
            for copy in result(n, k):
                copy.wait()
            for copy in first(n, k):
                copy.wait()


def backward(d0, zt, at, p, w1t, w2t, w1s, w2s, m1s, m2s, n_dev, cid=1):
    layers, d_ff, rows = zt.shape
    d_model = d0.shape[1]
    s1, s2 = d_model // n_dev, d_ff // n_dev
    sds = jax.ShapeDtypeStruct
    vm, sem = pltpu.VMEM, pltpu.SemaphoreType.DMA
    n_d, n_r = 2, 4
    scratch = [
        vm((rows, d_model), F32), vm((rows, d_model), BF16), vm((rows, d_ff), BF16),
        vm((2, d_ff, rows), BF16), vm((2, d_model, rows), BF16), vm((2, rows, d_ff), F32),
        vm((2, d_ff, d_model), BF16), vm((2, d_model, d_ff), BF16),
        vm((2, 2, 2, 2, s1, d_ff), BF16), vm((2, 2, 2, 2, s2, d_model), BF16),
        vm((n_d, 2, 2, s1, d_ff), BF16), vm((n_d, 2, 2, s2, d_model), BF16),
        vm((2, 2, 2, s1, d_ff), BF16), vm((2, 2, 2, s2, d_model), BF16),
        vm((n_r, 2, s1, d_ff), BF16), vm((n_r, 2, s2, d_model), BF16),
        vm((2, 2, s1, d_ff), BF16), vm((2, 2, s2, d_model), BF16),
        vm((n_r, s1, d_ff), BF16), vm((n_r, s2, d_model), BF16),
        vm((2, s1, d_ff), BF16), vm((2, s2, d_model), BF16),
        vm((2, s1, d_ff), BF16), vm((2, s2, d_model), BF16),
        vm((2, s1, d_ff), F32), vm((2, s2, d_model), F32), vm((2, s1, d_ff), F32), vm((2, s2, d_model), F32),
        sem((2, 5)), sem((2, 2, 2)), sem((2, 3)), sem(()), sem((n_d, 2)), sem((n_d, 2)), sem((n_r, 2)), sem((n_r, 2)),
        sem((n_r, 2)), sem((n_r, 2)), sem((2, 2, 2)),
    ]
    return pl.pallas_call(
        functools.partial(backward_kernel, layers),
        out_shape=(sds((layers, s1, d_ff), BF16), sds((layers, s2, d_model), BF16)) * 2 + (sds((PRE, 2, s1, d_ff), BF16),),
        in_specs=[ANY] * 10,
        out_specs=(ANY,) * 5,
        scratch_shapes=scratch,
        compiler_params=pltpu.CompilerParams(collective_id=cid, has_side_effects=True, vmem_limit_bytes=63 * 2**20),
        name="bwd",
    )(d0, zt, at, p, w1t, w2t, w1s, w2s, m1s, m2s)


def update_kernel(w1, w2, m1, m2, g1, g2, w1_out, w2_out, m1_out, m2_out):
    for w, m, g, w_out, m_out in ((w1, m1, g1, w1_out, m1_out), (w2, m2, g2, w2_out, m2_out)):
        mom = MOMENTUM * m[...] + g[...].astype(F32)
        m_out[...] = mom
        w_out[...] = w[...] - LEARN_RATE * mom


def update(w1, w2, m1, m2, g1, g2, block=8):
    spec = lambda v: pl.BlockSpec((block,) + v.shape[1:], lambda i: (i, 0, 0))
    args = (w1, w2, m1, m2, g1, g2)
    return pl.pallas_call(
        update_kernel,
        grid=(w1.shape[0] // block,),
        out_shape=tuple(jax.ShapeDtypeStruct(v.shape, F32) for v in args[:4]),
        in_specs=[spec(v) for v in args],
        out_specs=tuple(spec(v) for v in args[:4]),
        compiler_params=pltpu.CompilerParams(vmem_limit_bytes=63 * 2**20),
        cost_estimate=pl.CostEstimate(flops=8 * w1.size, bytes_accessed=36 * w1.size, transcendentals=0),
        name="update",
    )(*args)


def finish_kernel(h, y, h_out, loss_out):
    h_val = h[...]
    h_out[...] = h_val
    diff = h_val - y[...].astype(F32)
    loss_out[...] = jnp.sum(diff * diff, axis=1) / (2 * h.shape[1])


def finish(h, y, block=1536):
    rows, cols = h.shape
    spec = pl.BlockSpec((block, cols), lambda i: (i, 0))
    return pl.pallas_call(
        finish_kernel,
        grid=(rows // block,),
        out_shape=(jax.ShapeDtypeStruct(h.shape, F32), jax.ShapeDtypeStruct((rows,), F32)),
        in_specs=[spec, spec],
        out_specs=(spec, pl.BlockSpec((block,), lambda i: (i,))),
        cost_estimate=pl.CostEstimate(flops=3 * h.size, bytes_accessed=10 * h.size, transcendentals=0),
        name="finish",
    )(h, y)


def solution(mesh):
    n_dev = mesh.shape["data"]
    w_spec = P(None, "data", None)
    row_spec = P("data", None)

    def device_step(w_one, w_two, mom_one, mom_two, x_zero, y_zero, x_one, y_one):
        tok_dev, d_model = x_zero.shape
        scale = float(n_dev * tok_dev * d_model)
        d0, zt, at, p, w1t, w2t = forward(True, w_one, w_two, x_zero, y_zero, scale=scale, cid=0)
        g1, g2, low_one, low_two, first = backward(d0, zt, at, p, w1t, w2t, w_one, w_two, mom_one, mom_two, n_dev, cid=1)
        over_x = [(i, i + 2 - 4 * (i // 2 % 2)) for i in range(n_dev)]
        over_y = [(i, (i + 4) % n_dev) for i in range(n_dev)]
        given = [lax.ppermute(first, "data", perm) for perm in (over_x, over_y)]
        new_w_one, new_w_two, new_mom_one, new_mom_two = update(w_one, w_two, mom_one, mom_two, g1, g2)
        h_end = forward(False, low_one, low_two, x_one, *given, ahead=7, cid=2)
        h_last, loss_rows = finish(h_end, y_one)
        return new_w_one, new_w_two, new_mom_one, new_mom_two, loss_rows, h_last

    return jax.shard_map(device_step, mesh=mesh, in_specs=(w_spec, w_spec, w_spec, w_spec, row_spec, row_spec, row_spec, row_spec), out_specs=(w_spec, w_spec, w_spec, w_spec, P("data"), row_spec), check_vma=False)
```

```python
import functools

import jax
import jax.numpy as jnp
from jax import lax
from jax.experimental import pallas as pl
from jax.experimental.pallas import tpu as pltpu
from jax.sharding import PartitionSpec as P

LEARN_RATE = 0.1
MOMENTUM = 0.9
GELU_C = 0.7978845608028654
GELU_K = 0.044715
MESH = pl.DeviceIdType.MESH
F32 = jnp.float32
BF16 = jnp.bfloat16
AHEAD_CORE, AHEAD_RELAY = 1, 2
PRE = 5
EVAL_SLOTS = 9
CHUNK = 512
FIRST = (0, 3, 1, 4)
ANY = pl.BlockSpec(memory_space=pl.ANY)


def place():
    me = lax.axis_index("data")
    core, col, row = me % 2, (me // 2) % 2, me // 4
    return me, core, col, row


def index_of(row, col, core):
    return 4 * row + 2 * col + core


def greet(peers):
    barrier = pltpu.get_barrier_semaphore()
    for peer in peers:
        pl.semaphore_signal(barrier, inc=1, device_id=(peer,), device_id_type=MESH)
    return lambda: pl.semaphore_wait(barrier, len(peers))


def forward_kernel(train, layers, tile, scale, ahead, *refs):
    pre, slots = (0, ahead + 2) if train else (PRE, EVAL_SLOTS)
    eager, gone = (0, 0) if train else (3, PRE + 1)
    if train:
        (w1s, w2s, x_in, y_in, d_out, zt_out, at_out, p_out, w1_out, w2_out,
         w1, w2, h, xb, s1_st, s2_st, send_sem, recv_sem, own_sem, io_sem, out_sem,
         zt_st, at_st, p_st, st_sem, wt_sem) = refs
    else:
        (w1s, w2s, x_in, xs, ys, h_out, w1, w2, h, xb, s1_st, s2_st, send_sem, recv_sem, own_sem, io_sem, out_sem, pre_sem) = refs
    me, core, col, row = place()
    j_p = index_of(row, col, 1 - core)
    j_x = index_of(row, 1 - col, core)
    j_y = index_of(1 - row, col, core)
    j_d = index_of(1 - row, 1 - col, core)
    p_x = index_of(row, 1 - col, 1 - core)
    p_y = index_of(1 - row, col, 1 - core)
    p_d = index_of(1 - row, 1 - col, 1 - core)
    r1, r2 = w1s.shape[1], w2s.shape[1]
    rows = h.shape[0]
    tiles = rows // tile

    met = greet((j_p, j_x, j_y))

    def part(which, slot, j):
        if which == 1:
            return w1.at[slot, pl.ds(pl.multiple_of(j * r1, r1), r1)]
        return w2.at[slot, pl.ds(pl.multiple_of(j * r2, r2), r2)]

    sends = (
        (1, me, j_y, j_y), (1, me, j_x, j_x), (1, me, j_p, j_p),
        (2, me, j_x, j_x), (2, me, j_y, j_y), (2, me, j_p, j_p),
        (1, j_y, j_x, j_d), (1, j_y, j_p, p_y), (2, j_x, j_y, j_d), (2, j_x, j_p, p_x),
        (1, j_x, j_p, p_x), (2, j_y, j_p, p_y),
        (1, j_d, j_p, p_d), (2, j_d, j_p, p_d),
    )

    def channel(layer, k, incoming=False):
        slot = layer % slots
        which, out, to, inc = sends[k]
        ref = part(which, slot, inc if incoming else out)
        return pltpu.make_async_remote_copy(
            src_ref=ref, dst_ref=ref, send_sem=send_sem.at[slot, k], recv_sem=recv_sem.at[slot, k],
            device_id=(to,), device_id_type=MESH)

    def start(layer, ks):
        for k in ks:
            channel(layer, k).start()

    def arrive(layer, ks):
        for k in ks:
            channel(layer, k, True).wait_recv()

    def own(layer):
        st = layer % 2
        return (pltpu.make_async_copy(w1s.at[layer], s1_st.at[st], own_sem.at[st, 0]),
                pltpu.make_async_copy(w2s.at[layer], s2_st.at[st], own_sem.at[st, 1]))

    def given(layer):
        slot, half = layer % slots, w2.shape[2]
        copies = []
        for src, j in ((xs, j_x), (ys, j_y)):
            copies.append((src.at[layer, 0], part(1, slot, j)))
            for i in range(2):
                rows_2 = pl.ds(pl.multiple_of(j * r2 + i * r1, r1), r1)
                copies.append((src.at[layer, 1, :, pl.ds(i * half, half)], w2.at[slot, rows_2]))
        return tuple(pltpu.make_async_copy(src, dst, pre_sem.at[layer, k]) for k, (src, dst) in enumerate(copies))

    def place_own(layer):
        for copy in own(layer):
            copy.wait()
        part(1, layer % slots, me)[...] = s1_st[layer % 2].astype(BF16)
        part(2, layer % slots, me)[...] = s2_st[layer % 2].astype(BF16)

    def leave(layer):
        place_own(layer)

        @pl.when(layer >= pre)
        def _():
            start(layer, FIRST)

        start(layer, (2, 5))

    def relay(layer):
        if pre:
            @pl.when(layer < pre)
            def _():
                for copy in given(layer):
                    copy.wait()

        @pl.when(layer >= pre)
        def _():
            arrive(layer, FIRST)

        start(layer, (6, 8, 7, 9, 10, 11))

    def on(layer):
        return jnp.logical_and(layer >= 0, layer < layers)

    def gather(i):
        @pl.when(on(i + AHEAD_CORE))
        def _():
            arrive(i + AHEAD_CORE, (6, 8))
            start(i + AHEAD_CORE, (12, 13))

        @pl.when(jnp.logical_and(on(i + AHEAD_RELAY), i + AHEAD_RELAY >= eager))
        def _():
            relay(i + AHEAD_RELAY)

        @pl.when(jnp.logical_and(on(i + ahead), i + ahead >= gone))
        def _():
            leave(i + ahead)

        @pl.when(jnp.logical_and(on(i + ahead + 2), i + ahead >= gone))
        def _():
            for copy in own(i + ahead + 2):
                copy.start()

    def saved(layer, t, st):
        cols = pl.ds(pl.multiple_of(t * tile, tile), tile)
        return (pltpu.make_async_copy(zt_st.at[st], zt_out.at[layer, :, cols], st_sem.at[st, 0]),
                pltpu.make_async_copy(at_st.at[st], at_out.at[layer, :, cols], st_sem.at[st, 1]),
                pltpu.make_async_copy(p_st.at[st], p_out.at[layer, cols], st_sem.at[st, 2]))

    def final(t):
        where = pl.ds(t * tile, tile)
        return pltpu.make_async_copy(h.at[where], (d_out if train else h_out).at[where], out_sem.at[t])

    def kept(layer):
        slot = layer % slots
        return (pltpu.make_async_copy(w1.at[slot], w1_out.at[layer], wt_sem.at[0]),
                pltpu.make_async_copy(w2.at[slot], w2_out.at[layer], wt_sem.at[1]))

    def compute(layer):
        slot = layer % slots
        if train:
            for copy in kept(layer):
                copy.start()

        def one(t):
            where = pl.ds(t * tile, tile)
            h_val = h[where, :]
            a_val = h_val.astype(BF16)
            step = layer * tiles + t
            st = step % 2
            if train:
                @pl.when(step >= 2)
                def _():
                    for copy in saved((step - 2) // tiles, (step - 2) % tiles, st):
                        copy.wait()

                at_st[st] = a_val.T
            lows = []
            for c in range(0, w1.shape[2], CHUNK):
                cut = slice(c, c + CHUNK)
                u = jnp.dot(a_val, w1[slot, :, cut], preferred_element_type=F32)
                sq = u * u
                w = 0.5 * (1.0 + jnp.tanh(u * (GELU_C + (GELU_C * GELU_K) * sq)))
                z = u * w
                z_low = z.astype(BF16)
                lows.append(z_low)
                if train:
                    p_st[st, :, cut] = w + (z * (1.0 - w)) * (2.0 * GELU_C + (6.0 * GELU_C * GELU_K) * sq)
                    zt_st[st, cut, :] = z_low.T
            if train:
                for copy in saved(layer, t, st):
                    copy.start()
            z_low = jnp.concatenate(lows, axis=1)
            h[where, :] = h_val + jnp.dot(z_low, w2[slot], preferred_element_type=F32)

            @pl.when(layer == layers - 1)
            def _():
                if train:
                    if t == 0:
                        y_copy.wait()
                    h[where, :] = (h[where, :] - xb[where, :].astype(F32)) / scale
                final(t).start()

        one(0)
        gather(layer)
        for t in range(1, tiles):
            one(t)
        if train:
            for copy in kept(layer):
                copy.wait()

    x_copy = pltpu.make_async_copy(x_in, xb, io_sem.at[0])
    if train:
        y_copy = pltpu.make_async_copy(y_in, xb, io_sem.at[1])
    x_copy.start()
    for layer in (0, 1):
        for copy in own(layer):
            copy.start()
    for layer in range(pre):
        for copy in given(layer):
            copy.start()
    met()

    def widen(t, _):
        where = pl.ds(pl.multiple_of(t * 256, 256), 256)
        h[where, :] = xb[where, :].astype(F32)
        return 0

    def turn(n, _):
        i = n - ahead

        @pl.when(i < 0)
        def _():
            gather(i)

        @pl.when(i == -1)
        def _():
            x_copy.wait()
            lax.fori_loop(0, rows // 256, widen, 0)
            if train:
                y_copy.start()

        @pl.when(i >= 0)
        def _():
            arrive(i, (2, 5, 7, 9, 10, 11, 12, 13))
            compute(i)
            for k in range(len(sends)):
                if pre and k in FIRST:
                    @pl.when(i >= pre)
                    def _(k=k):
                        channel(i, k).wait_send()
                else:
                    channel(i, k).wait_send()

        return 0

    if not train:
        for layer in range(gone):
            leave(jnp.int32(layer))
            for copy in own(layer + 2):
                copy.start()
            if layer < eager:
                relay(jnp.int32(layer))
    lax.fori_loop(0 if train else ahead - 1, layers + ahead, turn, 0)

    if train:
        last = layers * tiles
        for step in (last - 2, last - 1):
            for copy in saved(step // tiles, step % tiles, step % 2):
                copy.wait()
    for t in range(tiles):
        final(t).wait()


def forward(train, w1s, w2s, x, *more, scale=None, tile=768, ahead=4, cid=0):
    slots = ahead + 2 if train else EVAL_SLOTS
    layers, r1, d_ff = w1s.shape
    r2, d_model = w2s.shape[1:]
    rows = x.shape[0]
    sds = jax.ShapeDtypeStruct
    h_shape = sds((rows, d_model), F32)
    scratch = [
        pltpu.VMEM((slots, d_model, d_ff), BF16), pltpu.VMEM((slots, d_ff, d_model), BF16),
        pltpu.VMEM((rows, d_model), F32), pltpu.VMEM((rows, d_model), BF16),
        pltpu.VMEM((2, r1, d_ff), w1s.dtype), pltpu.VMEM((2, r2, d_model), w2s.dtype),
        pltpu.SemaphoreType.DMA((slots, 14)), pltpu.SemaphoreType.DMA((slots, 14)),
        pltpu.SemaphoreType.DMA((2, 2)), pltpu.SemaphoreType.DMA((2,)), pltpu.SemaphoreType.DMA((rows // tile,)),
    ]
    out = h_shape
    args = (w1s, w2s, x, *more)
    if not train:
        scratch += [pltpu.SemaphoreType.DMA((PRE, 6))]
    if train:
        out = (h_shape, sds((layers, d_ff, rows), BF16), sds((layers, d_model, rows), BF16),
               sds((layers, rows, d_ff), F32), sds((layers, d_model, d_ff), BF16), sds((layers, d_ff, d_model), BF16))
        scratch += [
            pltpu.VMEM((2, d_ff, tile), BF16), pltpu.VMEM((2, d_model, tile), BF16), pltpu.VMEM((2, tile, d_ff), F32),
            pltpu.SemaphoreType.DMA((2, 3)), pltpu.SemaphoreType.DMA((2,)),
        ]
    return pl.pallas_call(
        functools.partial(forward_kernel, train, layers, tile, scale, ahead),
        out_shape=out,
        in_specs=[ANY] * len(args),
        out_specs=jax.tree.map(lambda _: ANY, out),
        scratch_shapes=scratch,
        compiler_params=pltpu.CompilerParams(collective_id=cid, has_side_effects=True, vmem_limit_bytes=60 * 2**20),
        name="fwd_train" if train else "fwd_eval",
    )(*args)


OVER_COLUMNS = (((1,), (1,)), ((), ()))


def backward_kernel(layers, *refs):
    (d_in, zt_in, at_in, p_in, w1_in, w2_in, w1s, w2s, m1s, m2s, g1_out, g2_out, nw1_out, nw2_out, first_out,
     d, db, r, zt, at, p, w1, w2, ga, gb, da, dbuf, sa, sb, ra, rb, ta, tb, fa, fb, oa, ob, na, nb, wa, wb, ma, mb,
     in_sem, own_sem, first_sem, d_sem, xd_send, xd_recv, x1_send, x1_recv, x2_send, x2_recv, out_sem) = refs
    me, core, col, row = place()
    j_p = index_of(row, col, 1 - core)
    j_x = index_of(row, 1 - col, core)
    j_y = index_of(1 - row, col, core)
    n_d, n_r = da.shape[0], ra.shape[0]
    s1, s2 = ga.shape[4], gb.shape[4]

    met = greet((j_p, j_x, j_y))

    def loads(n):
        layer, s = layers - 1 - n, n % 2
        return tuple(
            pltpu.make_async_copy(src.at[layer], dst.at[s], in_sem.at[s, k])
            for k, (src, dst) in enumerate(((zt_in, zt), (w2_in, w2), (p_in, p), (at_in, at), (w1_in, w1))))

    def remote(src, dst, send, recv, to):
        return pltpu.make_async_remote_copy(
            src_ref=src, dst_ref=dst, send_sem=send, recv_sem=recv, device_id=(to,), device_id_type=MESH)

    def hop_d(n, k):
        g, s = n % 2, n % n_d
        src, dst = ((ga, da), (gb, dbuf))[k]
        return remote(src.at[g, 1 - core], dst.at[s], xd_send.at[s, k], xd_recv.at[s, k], j_p)

    def hop_1(n, k):
        g, s = n % 2, n % n_r
        src, dst, away, to = ((sa, ra, 1 - row, j_y), (sb, rb, 1 - col, j_x))[k]
        return remote(src.at[g, away], dst.at[s], x1_send.at[s, k], x1_recv.at[s, k], to)

    def hop_2(n, k):
        g, s = n % 2, n % n_r
        src, dst, away, to = ((ta, fa, 1 - col, j_x), (tb, fb, 1 - row, j_y))[k]
        return remote(src.at[g, away], dst.at[s], x2_send.at[s, k], x2_recv.at[s, k], to)

    def result(n, k):
        s = n % 2
        pairs = (((oa, g1_out), (na, nw1_out)), ((ob, g2_out), (nb, nw2_out)))[k]
        return tuple(pltpu.make_async_copy(src.at[s], dst.at[layers - 1 - n], out_sem.at[s, k, i])
                     for i, (src, dst) in enumerate(pairs))

    def first(n, k):
        s, dst = n % 2, first_out.at[layers - 1 - n, k]
        if k == 0:
            return (pltpu.make_async_copy(na.at[s], dst, first_sem.at[s, 0]),)
        half = nb.shape[2]
        return tuple(
            pltpu.make_async_copy(nb.at[s, pl.ds(i * s1, s1)], dst.at[:, pl.ds(i * half, half)], first_sem.at[s, 1 + i])
            for i in range(2))

    def own(n, k):
        s = n % 2
        pairs = (((w1s, wa), (m1s, ma)), ((w2s, wb), (m2s, mb)))[k]
        return tuple(pltpu.make_async_copy(src.at[layers - 1 - n], dst.at[s], own_sem.at[s, k, i])
                     for i, (src, dst) in enumerate(pairs))

    def on(n):
        return jnp.logical_and(n >= 0, n < layers)

    def add(x, y):
        return (x.astype(F32) + y.astype(F32)).astype(BF16)

    def sum_core(m, k):
        @pl.when(on(m))
        def _():
            hop_d(m, k).wait()
            src, got, out = ((ga, da, sa), (gb, dbuf, sb))[k]
            out[m % 2] = add(src[m % 2, core], got[m % n_d])
            hop_1(m, k).start()

    def sum_first(m, k):
        @pl.when(on(m))
        def _():
            for copy in own(m, k):
                copy.start()
            hop_1(m, k).wait()
            src, got, out, here = ((sa, ra, ta, row), (sb, rb, tb, col))[k]
            out[m % 2] = add(src[m % 2, here], got[m % n_r])
            hop_2(m, k).start()

    def sum_second(m, k):
        @pl.when(on(m))
        def _():
            @pl.when(m >= 2)
            def _():
                for copy in result(m - 2, k):
                    copy.wait()

            @pl.when(m - 2 >= layers - PRE)
            def _():
                for copy in first(m - 2, k):
                    copy.wait()

            for copy in own(m, k):
                copy.wait()
            hop_2(m, k).wait()
            src, got, out, here = ((ta, fa, oa, col), (tb, fb, ob, row))[k]
            new, w, mom = ((na, wa, ma), (nb, wb, mb))[k]
            grad = add(src[m % 2, here], got[m % n_r])
            out[m % 2] = grad
            new_mom = MOMENTUM * mom[m % 2] + grad.astype(F32)
            new[m % 2] = (w[m % 2] - LEARN_RATE * new_mom).astype(BF16)
            for copy in result(m, k):
                copy.start()

            @pl.when(m >= layers - PRE)
            def _():
                for copy in first(m, k):
                    copy.start()

    def early(n):
        sum_second(n - 3, 1)
        sum_first(n - 2, 1)

    def late(n):
        sum_second(n - 3, 0)
        sum_first(n - 2, 0)
        sum_core(n, 1)

    def out_grad(n):
        s, g = n % 2, n % 2
        db[...] = d[...].astype(BF16)
        val = jnp.dot(zt[s], db[...], preferred_element_type=F32).astype(BF16)
        for k in range(8):
            gb[g, k % 2, (k // 2) % 2, k // 4] = val[k * s2:(k + 1) * s2]

    def in_back(n):
        s = n % 2
        q = lax.dot_general(db[...], w2[s], OVER_COLUMNS, preferred_element_type=F32)
        r[...] = (p[s] * q).astype(BF16)

    def state_back(n):
        @pl.when(n < layers - 1)
        def _():
            d[...] = d[...] + lax.dot_general(r[...], w1[n % 2], OVER_COLUMNS, preferred_element_type=F32)

    def in_grad(n):
        s, g = n % 2, n % 2
        val = jnp.dot(at[s], r[...], preferred_element_type=F32).astype(BF16)
        for k in range(8):
            ga[g, k % 2, k // 4, (k // 2) % 2] = val[k * s1:(k + 1) * s1]

    d_copy = pltpu.make_async_copy(d_in, d, d_sem)
    d_copy.start()
    for copy in loads(0):
        copy.start()
    met()
    d_copy.wait()

    def ready(n, ks):
        copies = loads(n)
        for k in ks:
            copies[k].wait()

    def turn(n, _):
        @pl.when(n < layers)
        def _():
            ready(n, (0,))
            out_grad(n)

        early(n)

        @pl.when(n < layers)
        def _():
            hop_d(n, 1).start()

            ready(n, (1, 2))

            @pl.when(n + 1 < layers)
            def _():
                for copy in loads(n + 1):
                    copy.start()

            in_back(n)

        late(n)

        @pl.when(n < layers)
        def _():
            ready(n, (3, 4))
            in_grad(n)
            hop_d(n, 0).start()
            state_back(n)

        sum_core(n, 0)
        return 0

    lax.fori_loop(0, layers + 3, turn, 0)
    for n in (layers - 2, layers - 1):
        for k in range(2):
            for copy in result(n, k):
                copy.wait()
            for copy in first(n, k):
                copy.wait()


def backward(d0, zt, at, p, w1, w2, w1s, w2s, m1s, m2s, n_dev, cid=1):
    layers, d_ff, rows = zt.shape
    d_model = d0.shape[1]
    s1, s2 = d_model // n_dev, d_ff // n_dev
    sds = jax.ShapeDtypeStruct
    vm, sem = pltpu.VMEM, pltpu.SemaphoreType.DMA
    n_d, n_r = 2, 4
    scratch = [
        vm((rows, d_model), F32), vm((rows, d_model), BF16), vm((rows, d_ff), BF16),
        vm((2, d_ff, rows), BF16), vm((2, d_model, rows), BF16), vm((2, rows, d_ff), F32),
        vm((2, d_model, d_ff), BF16), vm((2, d_ff, d_model), BF16),
        vm((2, 2, 2, 2, s1, d_ff), BF16), vm((2, 2, 2, 2, s2, d_model), BF16),
        vm((n_d, 2, 2, s1, d_ff), BF16), vm((n_d, 2, 2, s2, d_model), BF16),
        vm((2, 2, 2, s1, d_ff), BF16), vm((2, 2, 2, s2, d_model), BF16),
        vm((n_r, 2, s1, d_ff), BF16), vm((n_r, 2, s2, d_model), BF16),
        vm((2, 2, s1, d_ff), BF16), vm((2, 2, s2, d_model), BF16),
        vm((n_r, s1, d_ff), BF16), vm((n_r, s2, d_model), BF16),
        vm((2, s1, d_ff), BF16), vm((2, s2, d_model), BF16),
        vm((2, s1, d_ff), BF16), vm((2, s2, d_model), BF16),
        vm((2, s1, d_ff), F32), vm((2, s2, d_model), F32), vm((2, s1, d_ff), F32), vm((2, s2, d_model), F32),
        sem((2, 5)), sem((2, 2, 2)), sem((2, 3)), sem(()), sem((n_d, 2)), sem((n_d, 2)), sem((n_r, 2)), sem((n_r, 2)),
        sem((n_r, 2)), sem((n_r, 2)), sem((2, 2, 2)),
    ]
    return pl.pallas_call(
        functools.partial(backward_kernel, layers),
        out_shape=(sds((layers, s1, d_ff), BF16), sds((layers, s2, d_model), BF16)) * 2 + (sds((PRE, 2, s1, d_ff), BF16),),
        in_specs=[ANY] * 10,
        out_specs=(ANY,) * 5,
        scratch_shapes=scratch,
        compiler_params=pltpu.CompilerParams(collective_id=cid, has_side_effects=True, vmem_limit_bytes=63 * 2**20),
        name="bwd",
    )(d0, zt, at, p, w1, w2, w1s, w2s, m1s, m2s)


def update_kernel(w1, w2, m1, m2, g1, g2, w1_out, w2_out, m1_out, m2_out):
    for w, m, g, w_out, m_out in ((w1, m1, g1, w1_out, m1_out), (w2, m2, g2, w2_out, m2_out)):
        mom = MOMENTUM * m[...] + g[...].astype(F32)
        m_out[...] = mom
        w_out[...] = w[...] - LEARN_RATE * mom


def update(w1, w2, m1, m2, g1, g2, block=8):
    spec = lambda v: pl.BlockSpec((block,) + v.shape[1:], lambda i: (i, 0, 0))
    args = (w1, w2, m1, m2, g1, g2)
    return pl.pallas_call(
        update_kernel,
        grid=(w1.shape[0] // block,),
        out_shape=tuple(jax.ShapeDtypeStruct(v.shape, F32) for v in args[:4]),
        in_specs=[spec(v) for v in args],
        out_specs=tuple(spec(v) for v in args[:4]),
        compiler_params=pltpu.CompilerParams(vmem_limit_bytes=63 * 2**20),
        cost_estimate=pl.CostEstimate(flops=8 * w1.size, bytes_accessed=36 * w1.size, transcendentals=0),
        name="update",
    )(*args)


def finish_kernel(h, y, h_out, loss_out):
    h_val = h[...]
    h_out[...] = h_val
    diff = h_val - y[...].astype(F32)
    loss_out[...] = jnp.sum(diff * diff, axis=1) / (2 * h.shape[1])


def finish(h, y, block=1536):
    rows, cols = h.shape
    spec = pl.BlockSpec((block, cols), lambda i: (i, 0))
    return pl.pallas_call(
        finish_kernel,
        grid=(rows // block,),
        out_shape=(jax.ShapeDtypeStruct(h.shape, F32), jax.ShapeDtypeStruct((rows,), F32)),
        in_specs=[spec, spec],
        out_specs=(spec, pl.BlockSpec((block,), lambda i: (i,))),
        cost_estimate=pl.CostEstimate(flops=3 * h.size, bytes_accessed=10 * h.size, transcendentals=0),
        name="finish",
    )(h, y)


def solution(mesh):
    n_dev = mesh.shape["data"]
    w_spec = P(None, "data", None)
    row_spec = P("data", None)

    def device_step(w_one, w_two, mom_one, mom_two, x_zero, y_zero, x_one, y_one):
        tok_dev, d_model = x_zero.shape
        scale = float(n_dev * tok_dev * d_model)
        d0, zt, at, p, w1, w2 = forward(True, w_one, w_two, x_zero, y_zero, scale=scale, cid=0)
        g1, g2, low_one, low_two, first = backward(d0, zt, at, p, w1, w2, w_one, w_two, mom_one, mom_two, n_dev, cid=1)
        over_x = [(i, i + 2 - 4 * (i // 2 % 2)) for i in range(n_dev)]
        over_y = [(i, (i + 4) % n_dev) for i in range(n_dev)]
        given = [lax.ppermute(first, "data", perm) for perm in (over_x, over_y)]
        new_w_one, new_w_two, new_mom_one, new_mom_two = update(w_one, w_two, mom_one, mom_two, g1, g2)
        h_end = forward(False, low_one, low_two, x_one, *given, cid=2)
        h_last, loss_rows = finish(h_end, y_one)
        return new_w_one, new_w_two, new_mom_one, new_mom_two, loss_rows, h_last

    return jax.shard_map(device_step, mesh=mesh, in_specs=(w_spec, w_spec, w_spec, w_spec, row_spec, row_spec, row_spec, row_spec), out_specs=(w_spec, w_spec, w_spec, w_spec, P("data"), row_spec), check_vma=False)
```

```python
import functools

import jax
import jax.numpy as jnp
from jax import lax
from jax.experimental import pallas as pl
from jax.experimental.pallas import tpu as pltpu
from jax.sharding import PartitionSpec as P

LEARN_RATE = 0.1
MOMENTUM = 0.9
GELU_C = 0.7978845608028654
GELU_K = 0.044715
MESH = pl.DeviceIdType.MESH
F32 = jnp.float32
BF16 = jnp.bfloat16
AHEAD_CORE, AHEAD_RELAY = 1, 2
PRE = 5
EVAL_SLOTS = 9
CHUNK = 512
FIRST = (0, 3, 1, 4)
ANY = pl.BlockSpec(memory_space=pl.ANY)


def place():
    me = lax.axis_index("data")
    core, col, row = me % 2, (me // 2) % 2, me // 4
    return me, core, col, row


def index_of(row, col, core):
    return 4 * row + 2 * col + core


def greet(peers):
    barrier = pltpu.get_barrier_semaphore()
    for peer in peers:
        pl.semaphore_signal(barrier, inc=1, device_id=(peer,), device_id_type=MESH)
    return lambda: pl.semaphore_wait(barrier, len(peers))


def forward_kernel(train, layers, tile, scale, ahead, *refs):
    pre, slots = (0, ahead + 2) if train else (PRE, EVAL_SLOTS)
    eager, gone = (0, 0) if train else (3, PRE + 1)
    if train:
        (w1s, w2s, x_in, y_in, d_out, zt_out, at_out, p_out, w1_out, w2_out,
         w1, w2, h, xb, s1_st, s2_st, send_sem, recv_sem, own_sem, io_sem, out_sem,
         zt_st, at_st, p_st, st_sem, wt_sem) = refs
    else:
        (w1s, w2s, x_in, xs, ys, h_out, w1, w2, h, xb, s1_st, s2_st, send_sem, recv_sem, own_sem, io_sem, out_sem, pre_sem) = refs
    me, core, col, row = place()
    j_p = index_of(row, col, 1 - core)
    j_x = index_of(row, 1 - col, core)
    j_y = index_of(1 - row, col, core)
    j_d = index_of(1 - row, 1 - col, core)
    p_x = index_of(row, 1 - col, 1 - core)
    p_y = index_of(1 - row, col, 1 - core)
    p_d = index_of(1 - row, 1 - col, 1 - core)
    r1, r2 = w1s.shape[1], w2s.shape[1]
    rows = h.shape[0]
    tiles = rows // tile

    met = greet((j_p, j_x, j_y))

    def part(which, slot, j):
        if which == 1:
            return w1.at[slot, pl.ds(pl.multiple_of(j * r1, r1), r1)]
        return w2.at[slot, pl.ds(pl.multiple_of(j * r2, r2), r2)]

    sends = (
        (1, me, j_y, j_y), (1, me, j_x, j_x), (1, me, j_p, j_p),
        (2, me, j_x, j_x), (2, me, j_y, j_y), (2, me, j_p, j_p),
        (1, j_y, j_x, j_d), (1, j_y, j_p, p_y), (2, j_x, j_y, j_d), (2, j_x, j_p, p_x),
        (1, j_x, j_p, p_x), (2, j_y, j_p, p_y),
        (1, j_d, j_p, p_d), (2, j_d, j_p, p_d),
    )

    def channel(layer, k, incoming=False):
        slot = layer % slots
        which, out, to, inc = sends[k]
        ref = part(which, slot, inc if incoming else out)
        return pltpu.make_async_remote_copy(
            src_ref=ref, dst_ref=ref, send_sem=send_sem.at[slot, k], recv_sem=recv_sem.at[slot, k],
            device_id=(to,), device_id_type=MESH)

    def start(layer, ks):
        for k in ks:
            channel(layer, k).start()

    def arrive(layer, ks):
        for k in ks:
            channel(layer, k, True).wait_recv()

    def own(layer):
        st = layer % 2
        return (pltpu.make_async_copy(w1s.at[layer], s1_st.at[st], own_sem.at[st, 0]),
                pltpu.make_async_copy(w2s.at[layer], s2_st.at[st], own_sem.at[st, 1]))

    def given(layer):
        slot, half = layer % slots, w2.shape[2]
        copies = []
        for src, j in ((xs, j_x), (ys, j_y)):
            copies.append((src.at[layer, 0], part(1, slot, j)))
            for i in range(2):
                rows_2 = pl.ds(pl.multiple_of(j * r2 + i * r1, r1), r1)
                copies.append((src.at[layer, 1, :, pl.ds(i * half, half)], w2.at[slot, rows_2]))
        return tuple(pltpu.make_async_copy(src, dst, pre_sem.at[layer, k]) for k, (src, dst) in enumerate(copies))

    def place_own(layer):
        for copy in own(layer):
            copy.wait()
        part(1, layer % slots, me)[...] = s1_st[layer % 2].astype(BF16)
        part(2, layer % slots, me)[...] = s2_st[layer % 2].astype(BF16)

    def leave(layer):
        place_own(layer)

        @pl.when(layer >= pre)
        def _():
            start(layer, FIRST)

        start(layer, (2, 5))

    def relay(layer):
        if pre:
            @pl.when(layer < pre)
            def _():
                for copy in given(layer):
                    copy.wait()

        @pl.when(layer >= pre)
        def _():
            arrive(layer, FIRST)

        start(layer, (6, 8, 7, 9, 10, 11))

    def on(layer):
        return jnp.logical_and(layer >= 0, layer < layers)

    def gather(i):
        @pl.when(on(i + AHEAD_CORE))
        def _():
            arrive(i + AHEAD_CORE, (6, 8))
            start(i + AHEAD_CORE, (12, 13))

        @pl.when(jnp.logical_and(on(i + AHEAD_RELAY), i + AHEAD_RELAY >= eager))
        def _():
            relay(i + AHEAD_RELAY)

        @pl.when(jnp.logical_and(on(i + ahead), i + ahead >= gone))
        def _():
            leave(i + ahead)

        @pl.when(jnp.logical_and(on(i + ahead + 2), i + ahead >= gone))
        def _():
            for copy in own(i + ahead + 2):
                copy.start()

    def saved(layer, t, st):
        cols = pl.ds(pl.multiple_of(t * tile, tile), tile)
        return (pltpu.make_async_copy(zt_st.at[st], zt_out.at[layer, :, cols], st_sem.at[st, 0]),
                pltpu.make_async_copy(at_st.at[st], at_out.at[layer, :, cols], st_sem.at[st, 1]),
                pltpu.make_async_copy(p_st.at[st], p_out.at[layer, cols], st_sem.at[st, 2]))

    def final(t):
        where = pl.ds(t * tile, tile)
        return pltpu.make_async_copy(h.at[where], (d_out if train else h_out).at[where], out_sem.at[t])

    def kept(layer):
        slot = layer % slots
        return (pltpu.make_async_copy(w1.at[slot], w1_out.at[layer], wt_sem.at[0]),
                pltpu.make_async_copy(w2.at[slot], w2_out.at[layer], wt_sem.at[1]))

    def compute(layer):
        slot = layer % slots
        if train:
            for copy in kept(layer):
                copy.start()

        def one(t):
            where = pl.ds(t * tile, tile)
            h_val = h[where, :]
            a_val = h_val.astype(BF16)
            step = layer * tiles + t
            st = step % 2
            if train:
                @pl.when(step >= 2)
                def _():
                    for copy in saved((step - 2) // tiles, (step - 2) % tiles, st):
                        copy.wait()

                at_st[st] = a_val.T
            lows = []
            for c in range(0, w1.shape[2], CHUNK):
                cut = slice(c, c + CHUNK)
                u = jnp.dot(a_val, w1[slot, :, cut], preferred_element_type=F32)
                sq = u * u
                w = 0.5 * (1.0 + jnp.tanh(u * (GELU_C + (GELU_C * GELU_K) * sq)))
                z = u * w
                z_low = z.astype(BF16)
                lows.append(z_low)
                if train:
                    p_st[st, :, cut] = w + (z * (1.0 - w)) * (2.0 * GELU_C + (6.0 * GELU_C * GELU_K) * sq)
                    zt_st[st, cut, :] = z_low.T
            if train:
                for copy in saved(layer, t, st):
                    copy.start()
            z_low = jnp.concatenate(lows, axis=1)
            h[where, :] = h_val + jnp.dot(z_low, w2[slot], preferred_element_type=F32)

            @pl.when(layer == layers - 1)
            def _():
                if train:
                    if t == 0:
                        y_copy.wait()
                    h[where, :] = (h[where, :] - xb[where, :].astype(F32)) / scale
                final(t).start()

        one(0)
        gather(layer)
        for t in range(1, tiles):
            one(t)
        if train:
            for copy in kept(layer):
                copy.wait()

    x_copy = pltpu.make_async_copy(x_in, xb, io_sem.at[0])
    if train:
        y_copy = pltpu.make_async_copy(y_in, xb, io_sem.at[1])
    x_copy.start()
    for layer in (0, 1):
        for copy in own(layer):
            copy.start()
    for layer in range(pre):
        for copy in given(layer):
            copy.start()
    met()

    def widen(t, _):
        where = pl.ds(pl.multiple_of(t * 256, 256), 256)
        h[where, :] = xb[where, :].astype(F32)
        return 0

    def turn(n, _):
        i = n - ahead

        @pl.when(i < 0)
        def _():
            gather(i)

        @pl.when(i == -1)
        def _():
            x_copy.wait()
            lax.fori_loop(0, rows // 256, widen, 0)
            if train:
                y_copy.start()

        @pl.when(i >= 0)
        def _():
            arrive(i, (2, 5, 7, 9, 10, 11, 12, 13))
            compute(i)
            for k in range(len(sends)):
                if pre and k in FIRST:
                    @pl.when(i >= pre)
                    def _(k=k):
                        channel(i, k).wait_send()
                else:
                    channel(i, k).wait_send()

        return 0

    if not train:
        for layer in range(gone):
            leave(jnp.int32(layer))
            for copy in own(layer + 2):
                copy.start()
            if layer < eager:
                relay(jnp.int32(layer))
    lax.fori_loop(0 if train else ahead - 1, layers + ahead, turn, 0)

    if train:
        last = layers * tiles
        for step in (last - 2, last - 1):
            for copy in saved(step // tiles, step % tiles, step % 2):
                copy.wait()
    for t in range(tiles):
        final(t).wait()


def forward(train, w1s, w2s, x, *more, scale=None, tile=768, ahead=4, cid=0):
    slots = ahead + 2 if train else EVAL_SLOTS
    layers, r1, d_ff = w1s.shape
    r2, d_model = w2s.shape[1:]
    rows = x.shape[0]
    sds = jax.ShapeDtypeStruct
    h_shape = sds((rows, d_model), F32)
    scratch = [
        pltpu.VMEM((slots, d_model, d_ff), BF16), pltpu.VMEM((slots, d_ff, d_model), BF16),
        pltpu.VMEM((rows, d_model), F32), pltpu.VMEM((rows, d_model), BF16),
        pltpu.VMEM((2, r1, d_ff), w1s.dtype), pltpu.VMEM((2, r2, d_model), w2s.dtype),
        pltpu.SemaphoreType.DMA((slots, 14)), pltpu.SemaphoreType.DMA((slots, 14)),
        pltpu.SemaphoreType.DMA((2, 2)), pltpu.SemaphoreType.DMA((2,)), pltpu.SemaphoreType.DMA((rows // tile,)),
    ]
    out = h_shape
    args = (w1s, w2s, x, *more)
    if not train:
        scratch += [pltpu.SemaphoreType.DMA((PRE, 6))]
    if train:
        out = (h_shape, sds((layers, d_ff, rows), BF16), sds((layers, d_model, rows), BF16),
               sds((layers, rows, d_ff), F32), sds((layers, d_model, d_ff), BF16), sds((layers, d_ff, d_model), BF16))
        scratch += [
            pltpu.VMEM((2, d_ff, tile), BF16), pltpu.VMEM((2, d_model, tile), BF16), pltpu.VMEM((2, tile, d_ff), F32),
            pltpu.SemaphoreType.DMA((2, 3)), pltpu.SemaphoreType.DMA((2,)),
        ]
    return pl.pallas_call(
        functools.partial(forward_kernel, train, layers, tile, scale, ahead),
        out_shape=out,
        in_specs=[ANY] * len(args),
        out_specs=jax.tree.map(lambda _: ANY, out),
        scratch_shapes=scratch,
        compiler_params=pltpu.CompilerParams(collective_id=cid, has_side_effects=True, vmem_limit_bytes=60 * 2**20),
        name="fwd_train" if train else "fwd_eval",
    )(*args)


OVER_COLUMNS = (((1,), (1,)), ((), ()))


def backward_kernel(layers, *refs):
    (d_in, zt_in, at_in, p_in, w1_in, w2_in, w1s, w2s, m1s, m2s, g1_out, g2_out, nw1_out, nw2_out, first_out,
     d, db, r, zt, at, p, w1, w2, ga, gb, da, dbuf, sa, sb, ra, rb, ta, tb, fa, fb, oa, ob, na, nb, wa, wb, ma, mb,
     in_sem, own_sem, first_sem, d_sem, xd_send, xd_recv, x1_send, x1_recv, x2_send, x2_recv, out_sem) = refs
    me, core, col, row = place()
    j_p = index_of(row, col, 1 - core)
    j_x = index_of(row, 1 - col, core)
    j_y = index_of(1 - row, col, core)
    n_d, n_r = da.shape[0], ra.shape[0]
    s1, s2 = ga.shape[4], gb.shape[4]

    met = greet((j_p, j_x, j_y))

    def loads(n):
        layer, s = layers - 1 - n, n % 2
        return tuple(
            pltpu.make_async_copy(src.at[layer], dst.at[s], in_sem.at[s, k])
            for k, (src, dst) in enumerate(((zt_in, zt), (w2_in, w2), (p_in, p), (at_in, at), (w1_in, w1))))

    def remote(src, dst, send, recv, to):
        return pltpu.make_async_remote_copy(
            src_ref=src, dst_ref=dst, send_sem=send, recv_sem=recv, device_id=(to,), device_id_type=MESH)

    def hop_d(n, k):
        g, s = n % 2, n % n_d
        src, dst = ((ga, da), (gb, dbuf))[k]
        return remote(src.at[g, 1 - core], dst.at[s], xd_send.at[s, k], xd_recv.at[s, k], j_p)

    def hop_1(n, k):
        g, s = n % 2, n % n_r
        src, dst, away, to = ((sa, ra, 1 - row, j_y), (sb, rb, 1 - col, j_x))[k]
        return remote(src.at[g, away], dst.at[s], x1_send.at[s, k], x1_recv.at[s, k], to)

    def hop_2(n, k):
        g, s = n % 2, n % n_r
        src, dst, away, to = ((ta, fa, 1 - col, j_x), (tb, fb, 1 - row, j_y))[k]
        return remote(src.at[g, away], dst.at[s], x2_send.at[s, k], x2_recv.at[s, k], to)

    def result(n, k):
        s = n % 2
        pairs = (((oa, g1_out), (na, nw1_out)), ((ob, g2_out), (nb, nw2_out)))[k]
        return tuple(pltpu.make_async_copy(src.at[s], dst.at[layers - 1 - n], out_sem.at[s, k, i])
                     for i, (src, dst) in enumerate(pairs))

    def first(n, k):
        s, dst = n % 2, first_out.at[layers - 1 - n, k]
        if k == 0:
            return (pltpu.make_async_copy(na.at[s], dst, first_sem.at[s, 0]),)
        half = nb.shape[2]
        return tuple(
            pltpu.make_async_copy(nb.at[s, pl.ds(i * s1, s1)], dst.at[:, pl.ds(i * half, half)], first_sem.at[s, 1 + i])
            for i in range(2))

    def own(n, k):
        s = n % 2
        pairs = (((w1s, wa), (m1s, ma)), ((w2s, wb), (m2s, mb)))[k]
        return tuple(pltpu.make_async_copy(src.at[layers - 1 - n], dst.at[s], own_sem.at[s, k, i])
                     for i, (src, dst) in enumerate(pairs))

    def on(n):
        return jnp.logical_and(n >= 0, n < layers)

    def add(x, y):
        return x + y

    def sum_core(m, k):
        @pl.when(on(m))
        def _():
            hop_d(m, k).wait()
            src, got, out = ((ga, da, sa), (gb, dbuf, sb))[k]
            out[m % 2] = add(src[m % 2, core], got[m % n_d])
            hop_1(m, k).start()

    def sum_first(m, k):
        @pl.when(on(m))
        def _():
            for copy in own(m, k):
                copy.start()
            hop_1(m, k).wait()
            src, got, out, here = ((sa, ra, ta, row), (sb, rb, tb, col))[k]
            out[m % 2] = add(src[m % 2, here], got[m % n_r])
            hop_2(m, k).start()

    def sum_second(m, k):
        @pl.when(on(m))
        def _():
            @pl.when(m >= 2)
            def _():
                for copy in result(m - 2, k):
                    copy.wait()

            @pl.when(m - 2 >= layers - PRE)
            def _():
                for copy in first(m - 2, k):
                    copy.wait()

            for copy in own(m, k):
                copy.wait()
            hop_2(m, k).wait()
            src, got, out, here = ((ta, fa, oa, col), (tb, fb, ob, row))[k]
            new, w, mom = ((na, wa, ma), (nb, wb, mb))[k]
            grad = add(src[m % 2, here], got[m % n_r])
            out[m % 2] = grad
            new_mom = MOMENTUM * mom[m % 2] + grad.astype(F32)
            new[m % 2] = (w[m % 2] - LEARN_RATE * new_mom).astype(BF16)
            for copy in result(m, k):
                copy.start()

            @pl.when(m >= layers - PRE)
            def _():
                for copy in first(m, k):
                    copy.start()

    def early(n):
        sum_second(n - 3, 1)
        sum_first(n - 2, 1)

    def late(n):
        sum_second(n - 3, 0)
        sum_first(n - 2, 0)
        sum_core(n, 1)

    def out_grad(n):
        s, g = n % 2, n % 2
        db[...] = d[...].astype(BF16)
        val = jnp.dot(zt[s], db[...], preferred_element_type=F32).astype(BF16)
        for k in range(8):
            gb[g, k % 2, (k // 2) % 2, k // 4] = val[k * s2:(k + 1) * s2]

    def in_back(n):
        s = n % 2
        q = lax.dot_general(db[...], w2[s], OVER_COLUMNS, preferred_element_type=F32)
        r[...] = (p[s] * q).astype(BF16)

    def state_back(n):
        @pl.when(n < layers - 1)
        def _():
            d[...] = d[...] + lax.dot_general(r[...], w1[n % 2], OVER_COLUMNS, preferred_element_type=F32)

    def in_grad(n):
        s, g = n % 2, n % 2
        val = jnp.dot(at[s], r[...], preferred_element_type=F32).astype(BF16)
        for k in range(8):
            ga[g, k % 2, k // 4, (k // 2) % 2] = val[k * s1:(k + 1) * s1]

    d_copy = pltpu.make_async_copy(d_in, d, d_sem)
    d_copy.start()
    for copy in loads(0):
        copy.start()
    met()
    d_copy.wait()

    def ready(n, ks):
        copies = loads(n)
        for k in ks:
            copies[k].wait()

    def turn(n, _):
        @pl.when(n < layers)
        def _():
            ready(n, (0,))
            out_grad(n)

        early(n)

        @pl.when(n < layers)
        def _():
            hop_d(n, 1).start()

            ready(n, (1, 2))

            @pl.when(n + 1 < layers)
            def _():
                for copy in loads(n + 1):
                    copy.start()

            in_back(n)

        late(n)

        @pl.when(n < layers)
        def _():
            ready(n, (3, 4))
            in_grad(n)
            hop_d(n, 0).start()
            state_back(n)

        sum_core(n, 0)
        return 0

    lax.fori_loop(0, layers + 3, turn, 0)
    for n in (layers - 2, layers - 1):
        for k in range(2):
            for copy in result(n, k):
                copy.wait()
            for copy in first(n, k):
                copy.wait()


def backward(d0, zt, at, p, w1, w2, w1s, w2s, m1s, m2s, n_dev, cid=1):
    layers, d_ff, rows = zt.shape
    d_model = d0.shape[1]
    s1, s2 = d_model // n_dev, d_ff // n_dev
    sds = jax.ShapeDtypeStruct
    vm, sem = pltpu.VMEM, pltpu.SemaphoreType.DMA
    n_d, n_r = 2, 4
    scratch = [
        vm((rows, d_model), F32), vm((rows, d_model), BF16), vm((rows, d_ff), BF16),
        vm((2, d_ff, rows), BF16), vm((2, d_model, rows), BF16), vm((2, rows, d_ff), F32),
        vm((2, d_model, d_ff), BF16), vm((2, d_ff, d_model), BF16),
        vm((2, 2, 2, 2, s1, d_ff), BF16), vm((2, 2, 2, 2, s2, d_model), BF16),
        vm((n_d, 2, 2, s1, d_ff), BF16), vm((n_d, 2, 2, s2, d_model), BF16),
        vm((2, 2, 2, s1, d_ff), BF16), vm((2, 2, 2, s2, d_model), BF16),
        vm((n_r, 2, s1, d_ff), BF16), vm((n_r, 2, s2, d_model), BF16),
        vm((2, 2, s1, d_ff), BF16), vm((2, 2, s2, d_model), BF16),
        vm((n_r, s1, d_ff), BF16), vm((n_r, s2, d_model), BF16),
        vm((2, s1, d_ff), BF16), vm((2, s2, d_model), BF16),
        vm((2, s1, d_ff), BF16), vm((2, s2, d_model), BF16),
        vm((2, s1, d_ff), F32), vm((2, s2, d_model), F32), vm((2, s1, d_ff), F32), vm((2, s2, d_model), F32),
        sem((2, 5)), sem((2, 2, 2)), sem((2, 3)), sem(()), sem((n_d, 2)), sem((n_d, 2)), sem((n_r, 2)), sem((n_r, 2)),
        sem((n_r, 2)), sem((n_r, 2)), sem((2, 2, 2)),
    ]
    return pl.pallas_call(
        functools.partial(backward_kernel, layers),
        out_shape=(sds((layers, s1, d_ff), BF16), sds((layers, s2, d_model), BF16)) * 2 + (sds((PRE, 2, s1, d_ff), BF16),),
        in_specs=[ANY] * 10,
        out_specs=(ANY,) * 5,
        scratch_shapes=scratch,
        compiler_params=pltpu.CompilerParams(collective_id=cid, has_side_effects=True, vmem_limit_bytes=63 * 2**20),
        name="bwd",
    )(d0, zt, at, p, w1, w2, w1s, w2s, m1s, m2s)


def update_kernel(w1, w2, m1, m2, g1, g2, w1_out, w2_out, m1_out, m2_out):
    for w, m, g, w_out, m_out in ((w1, m1, g1, w1_out, m1_out), (w2, m2, g2, w2_out, m2_out)):
        mom = MOMENTUM * m[...] + g[...].astype(F32)
        m_out[...] = mom
        w_out[...] = w[...] - LEARN_RATE * mom


def update(w1, w2, m1, m2, g1, g2, block=8):
    spec = lambda v: pl.BlockSpec((block,) + v.shape[1:], lambda i: (i, 0, 0))
    args = (w1, w2, m1, m2, g1, g2)
    return pl.pallas_call(
        update_kernel,
        grid=(w1.shape[0] // block,),
        out_shape=tuple(jax.ShapeDtypeStruct(v.shape, F32) for v in args[:4]),
        in_specs=[spec(v) for v in args],
        out_specs=tuple(spec(v) for v in args[:4]),
        compiler_params=pltpu.CompilerParams(vmem_limit_bytes=63 * 2**20),
        cost_estimate=pl.CostEstimate(flops=8 * w1.size, bytes_accessed=36 * w1.size, transcendentals=0),
        name="update",
    )(*args)


def finish_kernel(h, y, h_out, loss_out):
    h_val = h[...]
    h_out[...] = h_val
    diff = h_val - y[...].astype(F32)
    loss_out[...] = jnp.sum(diff * diff, axis=1) / (2 * h.shape[1])


def finish(h, y, block=1536):
    rows, cols = h.shape
    spec = pl.BlockSpec((block, cols), lambda i: (i, 0))
    return pl.pallas_call(
        finish_kernel,
        grid=(rows // block,),
        out_shape=(jax.ShapeDtypeStruct(h.shape, F32), jax.ShapeDtypeStruct((rows,), F32)),
        in_specs=[spec, spec],
        out_specs=(spec, pl.BlockSpec((block,), lambda i: (i,))),
        cost_estimate=pl.CostEstimate(flops=3 * h.size, bytes_accessed=10 * h.size, transcendentals=0),
        name="finish",
    )(h, y)


def solution(mesh):
    n_dev = mesh.shape["data"]
    w_spec = P(None, "data", None)
    row_spec = P("data", None)

    def device_step(w_one, w_two, mom_one, mom_two, x_zero, y_zero, x_one, y_one):
        tok_dev, d_model = x_zero.shape
        scale = float(n_dev * tok_dev * d_model)
        d0, zt, at, p, w1, w2 = forward(True, w_one, w_two, x_zero, y_zero, scale=scale, cid=0)
        g1, g2, low_one, low_two, first = backward(d0, zt, at, p, w1, w2, w_one, w_two, mom_one, mom_two, n_dev, cid=1)
        over_x = [(i, i + 2 - 4 * (i // 2 % 2)) for i in range(n_dev)]
        over_y = [(i, (i + 4) % n_dev) for i in range(n_dev)]
        given = [lax.ppermute(first, "data", perm) for perm in (over_x, over_y)]
        new_w_one, new_w_two, new_mom_one, new_mom_two = update(w_one, w_two, mom_one, mom_two, g1, g2)
        h_end = forward(False, low_one, low_two, x_one, *given, cid=2)
        h_last, loss_rows = finish(h_end, y_one)
        return new_w_one, new_w_two, new_mom_one, new_mom_two, loss_rows, h_last

    return jax.shard_map(device_step, mesh=mesh, in_specs=(w_spec, w_spec, w_spec, w_spec, row_spec, row_spec, row_spec, row_spec), out_specs=(w_spec, w_spec, w_spec, w_spec, P("data"), row_spec), check_vma=False)
```
